256 devices in a mesh: gx: 16 (over z, core), gy: 4 (over x), gz: 4 (over y).
Axes of the slice: x: 4, y: 4, z: 8, core: 2. Of those that a mesh axis runs over, the one named last changes fastest.
Arguments:
- edge_state: bfloat16 [524288, 512], P(('gx', 'gy', 'gz')), may hold values from -6 to 6
- angle_weight: float32 [524288, 32], P(('gx', 'gy', 'gz')), may hold values from -6 to 6
- angle_bins: int32 [524288, 32], P(('gx', 'gy', 'gz')), may hold values from 0 to 15
- send_slots: int32 [16, 4, 4, 27, 32], P('gx', 'gy', 'gz'), may hold values from -1 to 2047, as said below
- fetch_index: int32 [524288], P(('gx', 'gy', 'gz')), may hold values from -1 to 2911, as said below
- down_weight: bfloat16 [2, 512, 64], replicated, may hold values from -0.25 to 0.25
- bilinear: bfloat16 [2, 1024, 64], replicated, may hold values from -0.1875 to 0.1875
- up_weight: bfloat16 [2, 64, 512], replicated, may hold values from -0.75 to 0.75
- first_dense: bfloat16 [2, 512, 512], replicated, may hold values from -0.25 to 0.25
- second_dense: bfloat16 [2, 512, 512], replicated, may hold values from -0.25 to 0.25
Outputs:
- edge_out: bfloat16 [524288, 512], P(('gx', 'gy', 'gz'))
The draws below stay inside these ranges and needn't reach their ends.
Inputs may be any that keep to these rules, and one draw needn't show every extreme that they name: `send_slots`: direction t = 9a + 3b + c stands for the neighbouring brick at offset (a - 1, b - 1, c - 1), periodic. Row t of a brick lists, in its first slots, local edges whose reverses lie in the brick at direction t; the rest hold -1; row 13 holds only -1. Every edge is listed at most once. Some direction of every brick is full. `fetch_index`: -1 marks an empty neighbour slot. A value below 2048 is the local edge that is the reverse; 2048 + t * 32 + r says that the reverse is listed in slot r of row 26 - t of send_slots of the brick at direction t, and that this brick's own edge is listed in slot r of row t of its own send_slots. Reverses are mutual, live edges have live reverses, and rev of an edge is another edge.
All inputs are finite; a program needn't handle non-finite values.
Results may differ from the reference program's by a relative error of at most 0.014.
Values may be sent and summed in bfloat16 or wider, within the bound.
No kernel may reach another device: no remote copies, remote signals or barrier semaphores. Data moves between devices by JAX's collectives and lax.ppermute only.
A program may use at most 128 MiB of HBM per device.

```python
from functools import partial
import jax
import jax.numpy as jnp
from jax import lax

D = 512
TRIP = 64
ANG = 16
NEIGH = 32
BLOCKS = 2
ATOMS_DEV = 64
EDGE_DEV = 2048
SLOTS = 32
BX = 16
BY = 4
BZ = 4
BRICKS = 256
EDGES = 524288


def graph_tables(key):
    base_key = jax.random.fold_in(key, 91)
    key_counts, key_self, key_order = jax.random.split(base_key, 3)
    bricks = BX * BY * BZ
    brick_id = jnp.arange(bricks, dtype=jnp.int32)
    direction = jnp.arange(27, dtype=jnp.int32)
    drawn_counts = jax.random.randint(key_counts, (bricks, 27), SLOTS // 4, SLOTS + 1, dtype=jnp.int32)
    drawn_counts = jnp.where(direction[None, :] == (brick_id % 13)[:, None], SLOTS, drawn_counts)
    coord_x = brick_id // (BY * BZ)
    coord_y = brick_id // BZ % BY
    coord_z = brick_id % BZ
    partner = ((coord_x[:, None] + direction[None, :] // 9 - 1) % BX * BY + (coord_y[:, None] + direction[None, :] // 3 % 3 - 1) % BY) * BZ + (coord_z[:, None] + direction[None, :] % 3 - 1) % BZ
    mirrored = drawn_counts[partner, 26 - direction[None, :]]
    inside = 2 * jax.random.randint(key_self, (bricks,), EDGE_DEV // 8, EDGE_DEV // 4 + 1, dtype=jnp.int32)
    counts = jnp.where(direction[None, :] < 13, drawn_counts, mirrored)
    counts = jnp.where(direction[None, :] == 13, inside[:, None], counts)
    starts = jnp.cumsum(counts, axis=1) - counts
    finish = starts + counts
    shuffled = jax.vmap(lambda sub_key: jax.random.permutation(sub_key, EDGE_DEV))(jax.random.split(key_order, bricks)).astype(jnp.int32)
    slot_rank = jnp.arange(SLOTS, dtype=jnp.int32)
    places = starts[:, :, None] + slot_rank[None, None, :]
    filled = (slot_rank[None, None, :] < counts[:, :, None]) & (direction[None, :, None] != 13)
    picked = jnp.take_along_axis(shuffled, jnp.clip(places, 0, EDGE_DEV - 1).reshape(bricks, 27 * SLOTS), axis=1).reshape(bricks, 27, SLOTS)
    send_table = jnp.where(filled, picked, -1)
    position = jnp.arange(EDGE_DEV, dtype=jnp.int32)
    group_of = jnp.sum((finish[:, None, :] <= position[None, :, None]).astype(jnp.int32), axis=2)
    group_safe = jnp.minimum(group_of, 26)
    offset = position[None, :] - jnp.take_along_axis(starts, group_safe, axis=1)
    partner_place = starts[:, 13][:, None] + jnp.bitwise_xor(offset, 1)
    local_pair = jnp.take_along_axis(shuffled, jnp.clip(partner_place, 0, EDGE_DEV - 1), axis=1)
    fetched = jnp.where(group_of == 13, local_pair, EDGE_DEV + group_safe * SLOTS + offset)
    fetched = jnp.where(group_of >= 27, -1, fetched)
    inverse = jnp.argsort(shuffled, axis=1)
    fetch_table = jnp.take_along_axis(fetched, inverse, axis=1)
    return (send_table.reshape(BX, BY, BZ, 27, SLOTS).astype(jnp.int32), fetch_table.reshape(bricks * EDGE_DEV).astype(jnp.int32))


def draw_send_slots(key, part):
    return graph_tables(key)[0]


def draw_fetch_index(key, part):
    return graph_tables(key)[1]


def touch_ends(drawn, stream_key, smallest, top_value):
    index_at = [jax.random.randint(jax.random.fold_in(stream_key, axis), (), 0, length) for axis, length in enumerate(drawn.shape)]
    longest = drawn.shape.index(max(drawn.shape))
    neighbour = index_at[:longest] + [(index_at[longest] + 1) % drawn.shape[longest]] + index_at[longest + 1:]
    return drawn.at[tuple(index_at)].set(smallest).at[tuple(neighbour)].set(top_value)


def block_levels(rng, extent, shards, smallest, top_value):
    def one(dim, parts):
        heights = jax.random.uniform(jax.random.fold_in(jax.random.fold_in(rng, 6), dim), (parts,), jnp.float32, smallest / len(shards), top_value / len(shards))
        return jnp.repeat(jnp.exp(heights), extent[dim] // parts).reshape((-1,) + (1,) * (len(extent) - dim - 1))

    level = one(*shards[0])
    for cut in shards[1:]:
        level = level * one(*cut)
    return level


def gaussian(rng, shape, spread, most, cuts=(), kind=jnp.bfloat16):
    gain = block_levels(rng, shape, cuts, -0.22, 0.18) if cuts else 1.0
    values = jax.random.normal(rng, shape, jnp.float32) * spread * gain
    return jnp.minimum(jnp.maximum(values, -most), most).astype(kind)


def setup_inputs(seed: int = 0) -> dict:
    keys = jax.random.split(jax.random.key(seed), 11)
    return {
        "edge_state": gaussian(keys[0], (EDGES, D), 1.0, 6.0, ((0, 256),)),
        "angle_weight": gaussian(keys[1], (EDGES, NEIGH), 1.0, 6.0, ((0, 256),), jnp.float32),
        "angle_bins": touch_ends(jax.random.randint(keys[2], (EDGES, NEIGH), 0, ANG), jax.random.fold_in(keys[2], 1), 0, ANG - 1).astype(jnp.int32),
        "send_slots": draw_send_slots(jax.random.fold_in(keys[10], 71), 0),
        "fetch_index": draw_fetch_index(jax.random.fold_in(keys[10], 71), 0),
        "down_weight": gaussian(keys[5], (BLOCKS, D, TRIP), D ** -0.5, 0.25),
        "bilinear": gaussian(keys[6], (BLOCKS, ANG * TRIP, TRIP), (ANG * TRIP) ** -0.5, 0.1875),
        "up_weight": gaussian(keys[7], (BLOCKS, TRIP, D), TRIP ** -0.5, 0.75),
        "first_dense": gaussian(keys[8], (BLOCKS, D, D), D ** -0.5, 0.25),
        "second_dense": gaussian(keys[9], (BLOCKS, D, D), D ** -0.5, 0.25),
    }


HALF_ROOT = 0.7071067811865476


def reverse_table(send_slots, fetch_index):
    senders = send_slots.reshape(BRICKS, 27, SLOTS)
    position = jnp.arange(EDGES, dtype=jnp.int32)
    brick_id = position // EDGE_DEV
    remote = jnp.maximum(fetch_index - EDGE_DEV, 0)
    direction = remote // SLOTS
    within = remote % SLOTS
    coord_x = brick_id // (BY * BZ)
    coord_y = (brick_id // BZ) % BY
    coord_z = brick_id % BZ
    source = (((coord_x + direction // 9 - 1) % BX) * BY + (coord_y + (direction // 3) % 3 - 1) % BY) * BZ + (coord_z + direction % 3 - 1) % BZ
    distant = source * EDGE_DEV + senders[source, 26 - direction, within]
    nearby = brick_id * EDGE_DEV + jnp.maximum(fetch_index, 0)
    reverse = jnp.where(fetch_index >= EDGE_DEV, distant, nearby).astype(jnp.int32)
    return reverse, fetch_index >= 0


def per_brick(function, *arrays):
    shaped = tuple(array.reshape((BRICKS, EDGE_DEV) + array.shape[1:]) for array in arrays)
    result = lax.map(lambda pieces: function(*pieces), shaped)
    return result.reshape((EDGES,) + result.shape[2:])


def fetch_rows(values, reverse, live_edge):
    return jnp.where(live_edge[:, None], values[reverse], jnp.zeros((), values.dtype))


def project_down(row_block, down_l):
    return jax.nn.silu(jnp.dot(row_block, down_l, preferred_element_type=jnp.float32)).astype(jnp.bfloat16)


def triplets(gathered, weight_rows, bin_rows, live_rows, bilinear_l, up_l):
    neighbours = gathered.reshape(ATOMS_DEV, NEIGH, TRIP).astype(jnp.float32)
    slot_ids = jnp.arange(NEIGH, dtype=jnp.int32)
    distinct = slot_ids[:, None] != slot_ids[None, :]
    kept_pairs = live_rows.reshape(ATOMS_DEV, 1, NEIGH) & distinct[None]
    chosen = bin_rows.reshape(ATOMS_DEV, NEIGH, NEIGH)[..., None] == jnp.arange(ANG, dtype=jnp.int32)
    coefficients = jnp.where(kept_pairs[..., None] & chosen, weight_rows.reshape(ATOMS_DEV, NEIGH, NEIGH)[..., None], jnp.float32(0.0)).astype(jnp.bfloat16)
    summed = jnp.einsum("akjb,ajc->akbc", coefficients.astype(jnp.float32), neighbours)
    summed = summed.astype(jnp.bfloat16).reshape(EDGE_DEV, ANG * TRIP)
    triplet_out = jnp.dot(summed, bilinear_l, preferred_element_type=jnp.float32).astype(jnp.bfloat16)
    return jax.nn.silu(jnp.dot(triplet_out, up_l, preferred_element_type=jnp.float32)).astype(jnp.bfloat16)


def residual(row_block, returned, live_rows, first_l, second_l):
    mixed_rows = ((row_block.astype(jnp.float32) + returned.astype(jnp.float32)) * HALF_ROOT).astype(jnp.bfloat16)
    inner_rows = jax.nn.silu(jnp.dot(mixed_rows, first_l, preferred_element_type=jnp.float32)).astype(jnp.bfloat16)
    updated = (mixed_rows.astype(jnp.float32) + jax.nn.silu(jnp.dot(inner_rows, second_l, preferred_element_type=jnp.float32))) * HALF_ROOT
    return jnp.where(live_rows[:, None], updated, jnp.float32(0.0)).astype(jnp.bfloat16)


def reference(edge_state, angle_weight, angle_bins, send_slots, fetch_index, down_weight, bilinear, up_weight, first_dense, second_dense):
    reverse, live_edge = reverse_table(send_slots, fetch_index)
    edge_rows = edge_state
    for section_index in range(BLOCKS):
        projected = per_brick(partial(project_down, down_l=down_weight[section_index]), edge_rows)
        gathered = fetch_rows(projected, reverse, live_edge)
        lifted = per_brick(partial(triplets, bilinear_l=bilinear[section_index], up_l=up_weight[section_index]), gathered, angle_weight, angle_bins, live_edge)
        returned = fetch_rows(lifted, reverse, live_edge)
        edge_rows = per_brick(partial(residual, first_l=first_dense[section_index], second_l=second_dense[section_index]), edge_rows, returned, live_edge)
    return edge_rows
```

```python
import jax
import jax.numpy as jnp
from jax import lax
from jax.experimental import pallas as pl
from jax.experimental.pallas import tpu as pltpu
from jax.sharding import PartitionSpec as P

HALF_ROOT = 0.7071067811865476
F32 = jnp.float32
BF16 = jnp.bfloat16
VMEM_LIMIT = 56 * 1024 * 1024


def silu(x):
    half = 0.5 * x
    return half + half * jnp.tanh(half)


def dot(a, b):
    return jnp.dot(a, b, preferred_element_type=F32)


def dot_t(a, b):
    return lax.dot_general(a, b, (((1,), (1,)), ((), ())), preferred_element_type=F32)


def from_behind(array, axis, by):
    length = lax.axis_size(axis)
    return lax.ppermute(array, axis, [(i, (i + by) % length) for i in range(length)])


def exchange(buffer):
    for dim, axis in ((0, "gx"), (1, "gy"), (2, "gz")):
        from_low = from_behind(lax.slice_in_dim(buffer, 2, 3, axis=dim), axis, 1)
        from_high = from_behind(lax.slice_in_dim(buffer, 0, 1, axis=dim), axis, -1)
        middle = lax.slice_in_dim(buffer, 1, 2, axis=dim)
        buffer = jnp.concatenate([from_low, middle, from_high], axis=dim)
    return buffer


def residual(rows, lifted, first, second):
    mixed = ((rows.astype(F32) + lifted) * HALF_ROOT).astype(BF16)
    inner = silu(dot(mixed, first)).astype(BF16)
    return (mixed.astype(F32) + silu(dot(inner, second))) * HALF_ROOT


def spread_rows(rows_ref, wide_ref):
    count = rows_ref.shape[0]
    step = 256
    for start in range(0, count, step):
        for c in range(4):
            wide_ref[pl.ds(4 * start + c, step, stride=4), :] = rows_ref[
                start : start + step, 128 * c : 128 * (c + 1)
            ].astype(F32)


def move_rows(count, unroll, step):
    def body(i, carry):
        base = i * unroll
        for k in range(unroll):
            step(base + k)
        return carry

    lax.fori_loop(0, count // unroll, body, 0)


def pack_kernel(send_ref, rows_ref, out_ref, wide_ref, packed_ref):
    slots = send_ref.shape[0]
    spread_rows(rows_ref, wide_ref)

    def step(s):
        source = pl.multiple_of(send_ref[s] * 4, 4)
        target = pl.multiple_of(s * 4, 4)
        packed_ref[pl.ds(target, 4), :] = wide_ref[pl.ds(source, 4), :]

    move_rows(slots, 16, step)
    out_ref[...] = packed_ref[...].astype(BF16)


def local_kernel(fetch_ref, rows_ref, out_ref, wide_ref):
    count = rows_ref.shape[0]
    quarter = count // 4
    spread_rows(rows_ref, wide_ref)

    def atom(i, carry):
        target = (i % 4) * quarter + (i // 4) * 32
        for k in range(32):
            source = pl.multiple_of(fetch_ref[i * 32 + k] * 4, 4)
            out_ref[pl.ds(pl.multiple_of((target + k) * 4, 4), 4), :] = wide_ref[
                pl.ds(source, 4), :
            ]
        return carry

    lax.fori_loop(0, count // 32, atom, 0)


def blocks_kernel(
    target_ref,
    arrived_ref,
    reverse_ref,
    weight_ref,
    bins_ref,
    down_ref,
    mixer_ref,
    up_ref,
    first_ref,
    second_ref,
    trip_ref,
    send_ref,
    arrived32_ref,
    rows_ref,
    wide_ref,
    summed_ref,
    packed_ref,
):
    slots = target_ref.shape[0]
    count = rows_ref.shape[0]
    quarter = count // 4
    groups = quarter // 32
    trip = up_ref.shape[1]
    angular = summed_ref.shape[1] // 256
    arrived32_ref[...] = arrived_ref[...].astype(F32)

    def place(s):
        target = pl.multiple_of(target_ref[s] * 4, 4)
        reverse_ref[pl.ds(target, 4), :] = arrived32_ref[
            pl.ds(pl.multiple_of(s * 4, 4), 4), :
        ]

    move_rows(slots, 16, place)
    for start in range(0, count, 256):
        for c in range(4):
            rows_ref[start : start + 256, 128 * c : 128 * (c + 1)] = reverse_ref[
                pl.ds(4 * start + c, 256, stride=4), :
            ].astype(BF16)
    trip_ref[count : count + 8, :] = jnp.zeros((8, 128), F32)
    lane_block = lax.broadcasted_iota(jnp.int32, (quarter, 4 * trip), 1) // trip
    for block in range(2):
        down = down_ref[block]
        down = jnp.concatenate([down, down, down, down], axis=0)
        for a in range(4):
            projected = silu(dot_t(rows_ref[a * quarter : (a + 1) * quarter, :], down))
            projected = jnp.where(lane_block == a, projected, 0.0).astype(BF16)
            for g in range(groups):
                wide_ref[g, 32 * a : 32 * (a + 1), :] = projected[32 * g : 32 * (g + 1), :]

        def group(g, carry):
            start = pl.multiple_of(g * 32, 32)
            weight = weight_ref[pl.ds(start, 32), :]
            bins = bins_ref[pl.ds(start, 32), :]
            chosen = [jnp.where(bins == b, weight, 0.0).astype(BF16) for b in range(angular)]
            sums = dot(jnp.concatenate(chosen, axis=0), wide_ref[g]).astype(BF16)
            for b in range(angular):
                summed_ref[pl.ds(start, 32), 256 * b : 256 * (b + 1)] = sums[
                    32 * b : 32 * (b + 1), :
                ]
            return carry

        lax.fori_loop(0, groups, group, 0)
        triplet = dot(summed_ref[...], mixer_ref[block]).astype(BF16)
        for a in range(4):
            part = triplet[:, trip * a : trip * (a + 1)]
            trip_ref[a * quarter : (a + 1) * quarter, trip * block : trip * (block + 1)] = (
                part.astype(F32)
            )
            if block == 0:
                lifted = silu(dot(part, up_ref[0])).astype(BF16).astype(F32)
                rows = rows_ref[a * quarter : (a + 1) * quarter, :]
                rows_ref[a * quarter : (a + 1) * quarter, :] = residual(
                    rows, lifted, first_ref[0], second_ref[0]
                ).astype(BF16)

    def pick(s):
        packed_ref[pl.ds(s, 1), :] = trip_ref[pl.ds(target_ref[s], 1), :]

    move_rows(slots, 16, pick)
    send_ref[...] = packed_ref[...].astype(BF16)


def trip_kernel(fetch_ref, trip_ref, out_ref):
    count = fetch_ref.shape[0]

    def step(e):
        out_ref[pl.ds(e, 1), :] = trip_ref[pl.ds(fetch_ref[e], 1), :]

    move_rows(count, 16, step)


def final_kernel(
    send_ref,
    arrived_ref,
    trip_ref,
    rows_ref,
    live_ref,
    up_ref,
    first_ref,
    second_ref,
    out_ref,
    arrived32_ref,
):
    slots = send_ref.shape[0]
    count = rows_ref.shape[0]
    trip = up_ref.shape[1]
    arrived32_ref[...] = arrived_ref[...].astype(F32)

    def place(s):
        trip_ref[pl.ds(send_ref[s], 1), :] = arrived32_ref[pl.ds(s, 1), :]

    move_rows(slots, 16, place)
    step = 256
    for start in range(0, count, step):
        rows = rows_ref[start : start + step, :]
        both = trip_ref[start : start + step, :].astype(BF16)
        for block in range(2):
            part = both[:, trip * block : trip * (block + 1)]
            lifted = silu(dot(part, up_ref[block])).astype(BF16).astype(F32)
            updated = residual(rows, lifted, first_ref[block], second_ref[block])
            rows = updated.astype(BF16)
        out_ref[start : start + step, :] = jnp.where(
            live_ref[start : start + step, :] > 0.0, updated, 0.0
        ).astype(BF16)


def prepare_kernel(
    weight_ref, bins_ref, live_ref, bilinear_ref, weight_out_ref, bins_out_ref, mixer_ref
):
    neigh = weight_ref.shape[0]
    groups = weight_ref.shape[1] // (4 * neigh)
    trip = bilinear_ref.shape[1]
    angular = bilinear_ref.shape[2] // trip
    row = lax.broadcasted_iota(jnp.int32, (neigh, 4 * neigh), 0)
    lane = lax.broadcasted_iota(jnp.int32, (neigh, 4 * neigh), 1)
    distinct = row != lane % neigh

    def turn(block):
        return jnp.concatenate(
            [block[:, neigh * a : neigh * (a + 1)].T for a in range(4)], axis=1
        )

    for g in range(groups):
        lanes = slice(4 * neigh * g, 4 * neigh * (g + 1))
        rows = slice(neigh * g, neigh * (g + 1))
        weight_out_ref[rows, :] = turn(weight_ref[:, lanes])
        kept = distinct & (live_ref[g : g + 1, :] >= 0)
        bins_out_ref[rows, :] = jnp.where(kept, turn(bins_ref[:, lanes]), -1)
    lane_block = lax.broadcasted_iota(jnp.int32, (trip, 4 * trip), 1) // trip
    for block in range(2):
        for b in range(angular):
            part = bilinear_ref[block, :, trip * b : trip * (b + 1)].astype(F32).T
            wide = jnp.concatenate([part] * 4, axis=1)
            for a in range(4):
                start = 4 * trip * b + trip * a
                mixer_ref[block, start : start + trip, :] = jnp.where(
                    lane_block == a, wide, 0.0
                ).astype(BF16)


def local(
    edge_state,
    angle_weight,
    angle_bins,
    send_slots,
    fetch_index,
    down_weight,
    bilinear,
    up_weight,
    first_dense,
    second_dense,
):
    count, width = edge_state.shape
    neigh = angle_weight.shape[1]
    trip = down_weight.shape[2]
    angular = bilinear.shape[1] // trip
    slots = 27 * send_slots.shape[-1]
    quarter = count // 4
    groups = count // (4 * neigh)
    spare = count + 8

    def turned(edges):
        return (edges // neigh % 4) * quarter + edges // (4 * neigh) * neigh + edges % neigh

    senders = send_slots.reshape(slots)
    send_rows = jnp.maximum(senders, 0)
    own_target = jnp.where(senders >= 0, senders, count)
    turned_target = jnp.where(senders >= 0, turned(send_rows), count)
    live = fetch_index >= 0
    is_local = live & (fetch_index < count)
    fetch_rows = jnp.where(is_local, fetch_index, 0)
    turned_fetch = jnp.where(is_local, turned(fetch_rows), count)
    live_column = live.astype(F32).reshape(count, 1)

    down_turned = jnp.swapaxes(down_weight, 1, 2)

    smem = pl.BlockSpec(memory_space=pltpu.SMEM)
    vmem = pl.BlockSpec(memory_space=pltpu.VMEM)
    params = pltpu.CompilerParams(vmem_limit_bytes=VMEM_LIMIT)

    packed = pl.pallas_call(
        pack_kernel,
        out_shape=jax.ShapeDtypeStruct((slots * 4, 128), BF16),
        in_specs=[smem, vmem],
        out_specs=vmem,
        scratch_shapes=[pltpu.VMEM((count * 4, 128), F32), pltpu.VMEM((slots * 4, 128), F32)],
        compiler_params=params,
        name="pack",
    )(send_rows, edge_state)
    weights, bins, mixer = pl.pallas_call(
        prepare_kernel,
        out_shape=(
            jax.ShapeDtypeStruct((quarter, 4 * neigh), F32),
            jax.ShapeDtypeStruct((quarter, 4 * neigh), jnp.int32),
            jax.ShapeDtypeStruct((2, angular * 4 * trip, 4 * trip), BF16),
        ),
        in_specs=[vmem] * 4,
        out_specs=(vmem, vmem, vmem),
        compiler_params=params,
        name="prepare",
    )(
        angle_weight.T,
        angle_bins.T,
        fetch_index.reshape(groups, 4 * neigh),
        jnp.swapaxes(bilinear, 1, 2),
    )
    arrived = exchange(packed.reshape(3, 3, 3, -1, 128)).reshape(slots * 4, 128)

    reverse = pl.pallas_call(
        local_kernel,
        out_shape=jax.ShapeDtypeStruct((spare * 4, 128), F32),
        in_specs=[smem, vmem],
        out_specs=vmem,
        scratch_shapes=[pltpu.VMEM((count * 4, 128), F32)],
        compiler_params=params,
        name="reverse_local",
    )(fetch_rows, edge_state)

    triplet, sending = pl.pallas_call(
        blocks_kernel,
        out_shape=(
            jax.ShapeDtypeStruct((spare, 2 * trip), F32),
            jax.ShapeDtypeStruct((slots, 2 * trip), BF16),
        ),
        in_specs=[smem] + [vmem] * 9,
        out_specs=(vmem, vmem),
        scratch_shapes=[
            pltpu.VMEM((slots * 4, 128), F32),
            pltpu.VMEM((count, width), BF16),
            pltpu.VMEM((groups, 4 * neigh, 4 * trip), BF16),
            pltpu.VMEM((quarter, angular * 4 * trip), BF16),
            pltpu.VMEM((slots, 2 * trip), F32),
        ],
        compiler_params=params,
        name="blocks",
    )(
        turned_target,
        arrived,
        reverse,
        weights,
        bins,
        down_turned,
        mixer,
        up_weight,
        first_dense,
        second_dense,
    )
    carried = exchange(sending.reshape(3, 3, 3, -1, 128)).reshape(slots, 2 * trip)

    own_trip = pl.pallas_call(
        trip_kernel,
        out_shape=jax.ShapeDtypeStruct((spare, 2 * trip), F32),
        in_specs=[smem, vmem],
        out_specs=vmem,
        compiler_params=params,
        name="trip_local",
    )(turned_fetch, triplet)

    out = pl.pallas_call(
        final_kernel,
        out_shape=jax.ShapeDtypeStruct((count, width), BF16),
        in_specs=[smem] + [vmem] * 7,
        out_specs=vmem,
        scratch_shapes=[pltpu.VMEM((slots, 2 * trip), F32)],
        compiler_params=params,
        name="final",
    )(
        own_target,
        carried,
        own_trip,
        edge_state,
        live_column,
        up_weight,
        first_dense,
        second_dense,
    )
    return out


def solution(mesh):
    spread = P(("gx", "gy", "gz"), None)
    in_specs = (
        spread,
        spread,
        spread,
        P("gx", "gy", "gz", None, None),
        P(("gx", "gy", "gz")),
        P(),
        P(),
        P(),
        P(),
        P(),
    )
    return jax.shard_map(local, mesh=mesh, in_specs=in_specs, out_specs=spread, check_vma=False)
```

```python
import jax
import jax.numpy as jnp
from jax import lax
from jax.experimental import pallas as pl
from jax.experimental.pallas import tpu as pltpu
from jax.sharding import PartitionSpec as P


HALF_ROOT = 0.7071067811865476
F32 = jnp.float32
BF16 = jnp.bfloat16
MIB = 1024 * 1024


def silu_of_half(half):
    return half + half * jnp.tanh(half)


def dot(a, b):
    return jnp.dot(a, b, preferred_element_type=F32)


def dot_t(a, b):
    return lax.dot_general(a, b, (((1,), (1,)), ((), ())), preferred_element_type=F32)


def from_behind(array, axis, by):
    length = lax.axis_size(axis)
    return lax.ppermute(array, axis, [(i, (i + by) % length) for i in range(length)])


def second_kernel(low_ref, middle_ref, high_ref, *out_refs):
    third = low_ref.shape[0] // 3
    for a, slab_ref in enumerate((low_ref, middle_ref, high_ref)):
        for b, out_ref in enumerate(out_refs):
            out_ref[third * a : third * (a + 1), :] = slab_ref[third * b : third * (b + 1), :]


def third_kernel(low_ref, middle_ref, high_ref, *out_refs):
    rows = low_ref.shape[0] // 9
    for b, slab_ref in enumerate((low_ref, middle_ref, high_ref)):
        for a in range(3):
            for c, out_ref in enumerate(out_refs):
                source, target = rows * (3 * a + c), rows * (3 * b + a)
                out_ref[target : target + rows, :] = slab_ref[source : source + rows, :]


def exchange(slabs):
    vmem = pl.BlockSpec(memory_space=pltpu.VMEM)

    def regroup(kernel, pieces):
        return pl.pallas_call(
            kernel,
            out_shape=[jax.ShapeDtypeStruct(piece.shape, piece.dtype) for piece in pieces],
            in_specs=[vmem] * 3,
            out_specs=[vmem] * 3,
            compiler_params=pltpu.CompilerParams(vmem_limit_bytes=4 * MIB),
            name="regroup",
        )(*pieces)

    def hop(sent, axis):
        low, middle, high = sent
        return [from_behind(high, axis, 1), middle, from_behind(low, axis, -1)]

    slabs = hop(slabs, "gx")
    slabs = hop(regroup(second_kernel, slabs), "gy")
    return hop(regroup(third_kernel, slabs), "gz")


def pipelined(blocks, stages):
    for step in range(blocks + len(stages) - 1):
        for depth in reversed(range(len(stages))):
            if 0 <= step - depth < blocks:
                stages[depth](step - depth)


def spread_rows(rows_ref, wide_ref, start, count):
    for c in range(4):
        wide_ref[pl.ds(4 * start + c, count, stride=4), :] = rows_ref[
            start : start + count, 128 * c : 128 * (c + 1)
        ].astype(F32)


def move_rows(count, unroll, step):
    def body(i, carry):
        base = i * unroll
        for k in range(unroll):
            step(base + k)
        return carry

    lax.fori_loop(0, count // unroll, body, 0)


def pack_kernel(
    send_hbm_ref,
    rows_hbm_ref,
    low_ref,
    middle_ref,
    high_ref,
    send_ref,
    rows_ref,
    wide_ref,
    packed_ref,
    copied,
    listed,
):
    count = rows_ref.shape[0]
    directions, _, each = send_ref.shape
    chunk = count // 8
    copies = [
        pltpu.make_async_copy(
            rows_hbm_ref.at[pl.ds(chunk * i, chunk), :],
            rows_ref.at[pl.ds(chunk * i, chunk), :],
            copied.at[i],
        )
        for i in range(8)
    ]
    slots = pltpu.make_async_copy(send_hbm_ref, send_ref, listed)
    slots.start()
    for copy in copies:
        copy.start()
    for i, copy in enumerate(copies):
        copy.wait()
        spread_rows(rows_ref, wide_ref, chunk * i, chunk)
    slots.wait()

    def direction(t, carry):
        for r in range(each):
            source = pl.multiple_of(jnp.maximum(send_ref[t, 0, r], 0) * 4, 4)
            target = pl.multiple_of(t * (4 * each) + 4 * r, 4)
            packed_ref[pl.ds(target, 4), :] = wide_ref[pl.ds(source, 4), :]
        return carry

    lax.fori_loop(0, directions, direction, 0)
    slab = 9 * 4 * each
    for i, out_ref in enumerate((low_ref, middle_ref, high_ref)):
        out_ref[...] = packed_ref[slab * i : slab * (i + 1), :].astype(BF16)


def local_kernel(fetch_ref, rows_ref, out_ref, wide_ref):
    count = rows_ref.shape[0]
    quarter = count // 4
    for start in range(0, count, 256):
        spread_rows(rows_ref, wide_ref, start, 256)

    def atom(i, carry):
        target = (i % 4) * quarter + (i // 4) * 32
        for k in range(32):
            source = pl.multiple_of(fetch_ref[i * 32 + k] * 4, 4)
            out_ref[pl.ds(pl.multiple_of((target + k) * 4, 4), 4), :] = wide_ref[
                pl.ds(source, 4), :
            ]
        return carry

    lax.fori_loop(0, count // 32, atom, 0)


def widen_arrived(pieces, wide_ref):
    for c, piece in enumerate(pieces):
        rows = piece.shape[0] // 9
        for i in range(9):
            start = rows * (9 * (i % 3) + 3 * (i // 3) + c)
            wide_ref[start : start + rows, :] = piece[rows * i : rows * (i + 1), :].astype(F32)


def blocks_kernel(
    target_ref,
    low_ref,
    middle_ref,
    high_ref,
    reverse_ref,
    weight_ref,
    bins_ref,
    down_ref,
    mixer_ref,
    up_ref,
    first_ref,
    second_ref,
    trip_ref,
    send_low_ref,
    send_middle_ref,
    send_high_ref,
    arrived32_ref,
    rows_ref,
    wide_ref,
    summed_ref,
    packed_ref,
    mixed_ref,
    inner_ref,
):
    slots = target_ref.shape[0]
    count = rows_ref.shape[0]
    quarter = count // 4
    groups = quarter // 32
    trip = up_ref.shape[1]
    angular = summed_ref.shape[1] // 256
    widen_arrived((low_ref, middle_ref, high_ref), arrived32_ref)

    def place(s):
        target = pl.multiple_of(target_ref[s] * 4, 4)
        reverse_ref[pl.ds(target, 4), :] = arrived32_ref[pl.ds(pl.multiple_of(s * 4, 4), 4), :]

    move_rows(slots, 16, place)
    for start in range(0, count, 256):
        for c in range(4):
            rows_ref[start : start + 256, 128 * c : 128 * (c + 1)] = reverse_ref[
                pl.ds(4 * start + c, 256, stride=4), :
            ].astype(BF16)
    trip_ref[count : count + 8, :] = jnp.zeros((8, 128), F32)
    lane_block = lax.broadcasted_iota(jnp.int32, (256, 4 * trip), 1) // trip
    step = 256
    for block in range(2):
        down = down_ref[block]
        down = jnp.concatenate([down, down, down, down], axis=0)

        def project(i):
            start = step * i
            a = start // quarter
            half = dot_t(rows_ref[start : start + step, :], down)
            projected = jnp.where(lane_block == a, silu_of_half(half), 0.0).astype(BF16)
            for k in range(step // 32):
                g = (start % quarter) // 32 + k
                wide_ref[g, 32 * a : 32 * (a + 1), :] = projected[32 * k : 32 * (k + 1), :]

        if block == 0:
            for i in range(count // step):
                project(i)

        def group(g, carry):
            start = pl.multiple_of(g * 32, 32)
            weight = weight_ref[pl.ds(start, 32), :]
            bins = bins_ref[pl.ds(start, 32), :]
            zero = jnp.zeros_like(weight)
            chosen = [jnp.where(bins == b, weight, zero) for b in range(angular)]
            sums = dot(jnp.concatenate(chosen, axis=0), wide_ref[g]).astype(BF16)
            for b in range(angular):
                summed_ref[pl.ds(start, 32), 256 * b : 256 * (b + 1)] = sums[
                    32 * b : 32 * (b + 1), :
                ]
            return carry

        lax.fori_loop(0, groups, group, 0, unroll=4)
        triplet = dot(summed_ref[...], mixer_ref[block]).astype(BF16)
        for a in range(4):
            part = triplet[:, trip * a : trip * (a + 1)]
            trip_ref[a * quarter : (a + 1) * quarter, trip * block : trip * (block + 1)] = (
                part.astype(F32)
            )
        if block == 0:

            def lift(i):
                start = step * i
                a, low = start // quarter, start % quarter
                lifted = silu_of_half(
                    dot(triplet[low : low + step, trip * a : trip * (a + 1)], up_ref[0])
                )
                rows = rows_ref[start : start + step, :].astype(F32)
                mixed_ref[start : start + step, :] = ((rows + lifted) * HALF_ROOT).astype(BF16)

            def first(i):
                at = slice(step * i, step * (i + 1))
                inner_ref[at, :] = silu_of_half(dot(mixed_ref[at, :], first_ref[0])).astype(BF16)

            def second(i):
                at = slice(step * i, step * (i + 1))
                change = silu_of_half(dot(inner_ref[at, :], second_ref[0]))
                rows_ref[at, :] = ((mixed_ref[at, :].astype(F32) + change) * HALF_ROOT).astype(
                    BF16
                )

            next_down = jnp.concatenate([down_ref[1]] * 4, axis=0)

            def project_next(i):
                start = step * i
                a = start // quarter
                half = dot_t(rows_ref[start : start + step, :], next_down)
                projected = jnp.where(lane_block == a, silu_of_half(half), 0.0).astype(BF16)
                for k in range(step // 32):
                    g = (start % quarter) // 32 + k
                    wide_ref[g, 32 * a : 32 * (a + 1), :] = projected[32 * k : 32 * (k + 1), :]

            pipelined(count // step, (lift, first, second, project_next))

    def pick(s):
        packed_ref[pl.ds(s, 1), :] = trip_ref[pl.ds(target_ref[s], 1), :]

    move_rows(slots, 16, pick)
    slab = slots // 3
    for i, send_ref in enumerate((send_low_ref, send_middle_ref, send_high_ref)):
        send_ref[...] = packed_ref[slab * i : slab * (i + 1), :].astype(BF16)


def trip_kernel(fetch_ref, trip_ref, out_ref):
    count = fetch_ref.shape[0]

    def step(e):
        out_ref[pl.ds(e, 1), :] = trip_ref[pl.ds(fetch_ref[e], 1), :]

    move_rows(count, 16, step)


def final_kernel(
    send_ref,
    low_ref,
    middle_ref,
    high_ref,
    trip_ref,
    rows_ref,
    live_ref,
    up_ref,
    first_ref,
    second_ref,
    out_ref,
    arrived32_ref,
    mixed_ref,
    inner_ref,
    mixed_next_ref,
    inner_next_ref,
    rows_out_ref,
    mask_ref,
    copied,
):
    slots = send_ref.shape[0]
    count = rows_ref.shape[0]
    trip = up_ref.shape[1]
    widen_arrived((low_ref, middle_ref, high_ref), arrived32_ref)

    def place(s):
        trip_ref[pl.ds(send_ref[s], 1), :] = arrived32_ref[pl.ds(s, 1), :]

    move_rows(slots, 16, place)
    step = 256

    def lifted(at, block):
        both = trip_ref[at, :].astype(BF16)
        return silu_of_half(dot(both[:, trip * block : trip * (block + 1)], up_ref[block]))

    def lift(i):
        at = slice(step * i, step * (i + 1))
        for g in range(step * i // 128, step * (i + 1) // 128):
            line = live_ref[g : g + 1, :].astype(F32)
            mask_ref[128 * g : 128 * (g + 1), :] = jnp.broadcast_to(line, (128, 128)).T
        rows = rows_ref[at, :].astype(F32)
        mixed_ref[at, :] = ((rows + lifted(at, 0)) * HALF_ROOT).astype(BF16)

    def first(i):
        at = slice(step * i, step * (i + 1))
        inner_ref[at, :] = silu_of_half(dot(mixed_ref[at, :], first_ref[0])).astype(BF16)

    def second(i):
        at = slice(step * i, step * (i + 1))
        change = silu_of_half(dot(inner_ref[at, :], second_ref[0]))
        rows = (mixed_ref[at, :].astype(F32) + change) * HALF_ROOT
        mixed_next_ref[at, :] = ((rows + lifted(at, 1)) * HALF_ROOT).astype(BF16)

    def first_next(i):
        at = slice(step * i, step * (i + 1))
        inner_next_ref[at, :] = silu_of_half(dot(mixed_next_ref[at, :], first_ref[1])).astype(BF16)

    def second_next(i):
        at = slice(step * i, step * (i + 1))
        change = silu_of_half(dot(inner_next_ref[at, :], second_ref[1]))
        rows = (mixed_next_ref[at, :].astype(F32) + change) * HALF_ROOT
        for c in range(4):
            lanes = slice(128 * c, 128 * (c + 1))
            rows_out_ref[at, lanes] = jnp.where(mask_ref[at, :] >= 0.0, rows[:, lanes], 0.0).astype(
                BF16
            )
        copies[i].start()

    copies = [
        pltpu.make_async_copy(
            rows_out_ref.at[pl.ds(step * i, step), :],
            out_ref.at[pl.ds(step * i, step), :],
            copied.at[i],
        )
        for i in range(count // step)
    ]
    pipelined(count // step, (lift, first, second, first_next, second_next))
    for copy in copies:
        copy.wait()


def prepare_kernel(
    weight_ref,
    bins_ref,
    live_ref,
    bilinear_ref,
    up_ref,
    first_ref,
    second_ref,
    down_ref,
    weight_out_ref,
    bins_out_ref,
    mixer_ref,
    up_out_ref,
    first_out_ref,
    second_out_ref,
    down_out_ref,
):
    neigh = weight_ref.shape[0]
    side = 4 * neigh
    groups = weight_ref.shape[1] // side
    trip = bilinear_ref.shape[1]
    angular = bilinear_ref.shape[2] // trip
    row = lax.broadcasted_iota(jnp.int32, (side, side), 0)
    lane = lax.broadcasted_iota(jnp.int32, (side, side), 1)
    distinct = row % neigh != lane % neigh
    piece = lax.broadcasted_iota(jnp.int32, (neigh, side), 1) // neigh

    def turn(blocks):
        stacked = []
        for a in range(4):
            rows = jnp.zeros((neigh, side), F32)
            for h in range(4):
                shift = (h - a) * neigh % side
                moved = pltpu.roll(blocks[h], shift, 1) if shift else blocks[h]
                rows = jnp.where(piece == h, moved, rows)
            stacked.append(rows)
        return jnp.concatenate(stacked, axis=0).T

    for start in range(0, groups, 4):
        spans = [slice(side * (start + h), side * (start + h + 1)) for h in range(4)]
        rows = slice(neigh * start, neigh * start + side)
        weight_out_ref[rows, :] = turn([weight_ref[:, span] for span in spans]).astype(BF16)
        live = jnp.concatenate(
            [
                jnp.broadcast_to(live_ref[start + h : start + h + 1, :], (neigh, side))
                for h in range(4)
            ],
            axis=0,
        )
        bins = turn([bins_ref[:, span].astype(F32) for span in spans])
        bins_out_ref[rows, :] = jnp.where(distinct & (live >= 0), bins, -1.0).astype(BF16)
    lane_block = lax.broadcasted_iota(jnp.int32, (trip, 4 * trip), 1) // trip
    for block in range(2):
        turned = bilinear_ref[block].astype(F32).T
        wide = jnp.concatenate([turned] * 4, axis=1)
        for b in range(angular):
            part = wide[trip * b : trip * (b + 1), :]
            for a in range(4):
                start = 4 * trip * b + trip * a
                mixer_ref[block, start : start + trip, :] = jnp.where(
                    lane_block == a, part, 0.0
                ).astype(BF16)
    for source, target in (
        (up_ref, up_out_ref),
        (first_ref, first_out_ref),
        (second_ref, second_out_ref),
        (down_ref, down_out_ref),
    ):
        target[...] = (source[...].astype(F32) * 0.5).astype(BF16)


def local(
    edge_state,
    angle_weight,
    angle_bins,
    send_slots,
    fetch_index,
    down_weight,
    bilinear,
    up_weight,
    first_dense,
    second_dense,
):
    count, width = edge_state.shape
    neigh = angle_weight.shape[1]
    trip = down_weight.shape[2]
    angular = bilinear.shape[1] // trip
    slots = 27 * send_slots.shape[-1]
    quarter = count // 4
    groups = count // (4 * neigh)
    spare = count + 8

    def turned(edges):
        return (edges // neigh % 4) * quarter + edges // (4 * neigh) * neigh + edges % neigh

    senders = send_slots.reshape(slots)
    send_rows = jnp.maximum(senders, 0)
    own_target = jnp.where(senders >= 0, senders, count)
    turned_target = jnp.where(senders >= 0, turned(send_rows), count)
    live = fetch_index >= 0
    is_local = live & (fetch_index < count)
    fetch_rows = jnp.where(is_local, fetch_index, 0)
    turned_fetch = jnp.where(is_local, turned(fetch_rows), count)
    live_lines = fetch_index.reshape(groups, 4 * neigh)

    down_turned = jnp.swapaxes(down_weight, 1, 2)

    smem = pl.BlockSpec(memory_space=pltpu.SMEM)
    vmem = pl.BlockSpec(memory_space=pltpu.VMEM)

    def params(mib):
        return pltpu.CompilerParams(vmem_limit_bytes=mib * MIB)

    outside = pl.BlockSpec(memory_space=pltpu.HBM)
    slab = slots // 3
    each = send_slots.shape[-1]
    packed = pl.pallas_call(
        pack_kernel,
        out_shape=(jax.ShapeDtypeStruct((slab * 4, 128), BF16),) * 3,
        in_specs=[outside, outside],
        out_specs=(vmem,) * 3,
        scratch_shapes=[
            pltpu.SMEM((27, 1, each), jnp.int32),
            pltpu.VMEM((count, width), BF16),
            pltpu.VMEM((count * 4, 128), F32),
            pltpu.VMEM((slots * 4, 128), F32),
            pltpu.SemaphoreType.DMA((8,)),
            pltpu.SemaphoreType.DMA,
        ],
        compiler_params=params(14),
        name="pack",
    )(send_slots.reshape(27, 1, each), edge_state)
    weights, bins, mixer, up_half, first_half, second_half, down_half = pl.pallas_call(
        prepare_kernel,
        out_shape=(
            jax.ShapeDtypeStruct((quarter, 4 * neigh), BF16),
            jax.ShapeDtypeStruct((quarter, 4 * neigh), BF16),
            jax.ShapeDtypeStruct((2, angular * 4 * trip, 4 * trip), BF16),
            jax.ShapeDtypeStruct(up_weight.shape, BF16),
            jax.ShapeDtypeStruct(first_dense.shape, BF16),
            jax.ShapeDtypeStruct(second_dense.shape, BF16),
            jax.ShapeDtypeStruct(down_turned.shape, BF16),
        ),
        in_specs=[vmem] * 8,
        out_specs=(vmem,) * 7,
        compiler_params=params(16),
        name="prepare",
    )(
        angle_weight.T,
        angle_bins.T,
        live_lines,
        jnp.swapaxes(bilinear, 1, 2),
        up_weight,
        first_dense,
        second_dense,
        down_turned,
    )
    arrived = exchange(packed)

    reverse = pl.pallas_call(
        local_kernel,
        out_shape=jax.ShapeDtypeStruct((spare * 4, 128), F32),
        in_specs=[smem, vmem],
        out_specs=vmem,
        scratch_shapes=[pltpu.VMEM((count * 4, 128), F32)],
        compiler_params=params(14),
        name="reverse_local",
    )(fetch_rows, edge_state)

    triplet, *sending = pl.pallas_call(
        blocks_kernel,
        out_shape=(
            jax.ShapeDtypeStruct((spare, 2 * trip), F32),
        )
        + (jax.ShapeDtypeStruct((slab, 2 * trip), BF16),) * 3,
        in_specs=[smem] + [vmem] * 11,
        out_specs=(vmem,) * 4,
        scratch_shapes=[
            pltpu.VMEM((slots * 4, 128), F32),
            pltpu.VMEM((count, width), BF16),
            pltpu.VMEM((groups, 4 * neigh, 4 * trip), BF16),
            pltpu.VMEM((quarter, angular * 4 * trip), BF16),
            pltpu.VMEM((slots, 2 * trip), F32),
            pltpu.VMEM((count, width), BF16),
            pltpu.VMEM((count, width), BF16),
        ],
        compiler_params=params(32),
        name="blocks",
    )(
        turned_target,
        *arrived,
        reverse,
        weights,
        bins,
        down_half,
        mixer,
        up_half,
        first_half,
        second_half,
    )
    own_trip = pl.pallas_call(
        trip_kernel,
        out_shape=jax.ShapeDtypeStruct((spare, 2 * trip), F32),
        in_specs=[smem, vmem],
        out_specs=vmem,
        compiler_params=params(5),
        name="trip_local",
    )(turned_fetch, triplet)
    carried = exchange(sending)

    out = pl.pallas_call(
        final_kernel,
        out_shape=jax.ShapeDtypeStruct((count, width), BF16),
        in_specs=[smem] + [vmem] * 9,
        out_specs=outside,
        scratch_shapes=[pltpu.VMEM((slots, 2 * trip), F32)]
        + [pltpu.VMEM((count, width), BF16)] * 5
        + [pltpu.VMEM((count, 128), F32)]
        + [pltpu.SemaphoreType.DMA((8,))],
        compiler_params=params(24),
        name="final",
    )(
        own_target,
        *carried,
        own_trip,
        edge_state,
        live_lines,
        up_half,
        first_half,
        second_half,
    )
    return out


def solution(mesh):
    spread = P(("gx", "gy", "gz"), None)
    in_specs = (
        spread,
        spread,
        spread,
        P("gx", "gy", "gz", None, None),
        P(("gx", "gy", "gz")),
        P(),
        P(),
        P(),
        P(),
        P(),
    )

    return jax.shard_map(local, mesh=mesh, in_specs=in_specs, out_specs=spread, check_vma=False)
```

```python
import jax
import jax.numpy as jnp
from jax import lax
from jax.experimental import pallas as pl
from jax.experimental.pallas import tpu as pltpu
from jax.sharding import PartitionSpec as P


HALF_ROOT = 0.7071067811865476
F32 = jnp.float32
BF16 = jnp.bfloat16
MIB = 1024 * 1024
BLOCK_TRIPS = 2
FINAL_TRIPS = 1


def silu_of_half(half):
    return half + half * jnp.tanh(half)


def dot(a, b):
    return jnp.dot(a, b, preferred_element_type=F32)


def dot_t(a, b):
    return lax.dot_general(a, b, (((1,), (1,)), ((), ())), preferred_element_type=F32)


def from_behind(array, axis, by):
    length = lax.axis_size(axis)
    return lax.ppermute(array, axis, [(i, (i + by) % length) for i in range(length)])


def second_kernel(low_ref, middle_ref, high_ref, *out_refs):
    third = low_ref.shape[0] // 3
    for a, slab_ref in enumerate((low_ref, middle_ref, high_ref)):
        for b, out_ref in enumerate(out_refs):
            out_ref[third * a : third * (a + 1), :] = slab_ref[third * b : third * (b + 1), :]


def third_kernel(low_ref, middle_ref, high_ref, *out_refs):
    rows = low_ref.shape[0] // 9
    for b, slab_ref in enumerate((low_ref, middle_ref, high_ref)):
        for a in range(3):
            for c, out_ref in enumerate(out_refs):
                source, target = rows * (3 * a + c), rows * (3 * b + a)
                out_ref[target : target + rows, :] = slab_ref[source : source + rows, :]


def exchange(slabs):
    vmem = pl.BlockSpec(memory_space=pltpu.VMEM)

    def regroup(kernel, pieces):
        return pl.pallas_call(
            kernel,
            out_shape=[jax.ShapeDtypeStruct(piece.shape, piece.dtype) for piece in pieces],
            in_specs=[vmem] * 3,
            out_specs=[vmem] * 3,
            compiler_params=pltpu.CompilerParams(vmem_limit_bytes=4 * MIB),
            name="regroup",
        )(*pieces)

    def hop(sent, axis):
        low, middle, high = sent
        return [from_behind(high, axis, 1), middle, from_behind(low, axis, -1)]

    slabs = hop(slabs, "gx")
    slabs = hop(regroup(second_kernel, slabs), "gy")
    return hop(regroup(third_kernel, slabs), "gz")


def pipelined(blocks, stages, trips):
    share = blocks // trips

    def trip(t, carry):
        for step in range(share + len(stages) - 1):
            for depth in reversed(range(len(stages))):
                if 0 <= step - depth < share:
                    stages[depth](t * share + step - depth)
        return carry

    if trips == 1:
        trip(0, 0)
    else:
        lax.fori_loop(0, trips, trip, 0)


def span(i, size):
    if isinstance(i, int):
        return slice(size * i, size * (i + 1))
    return pl.ds(pl.multiple_of(size * i, size), size)


def spread_rows(rows_ref, wide_ref, start, count, shift=0):
    for c in range(4):
        wide_ref[pl.ds(4 * (start + shift) + c, count, stride=4), :] = rows_ref[
            start : start + count, 128 * c : 128 * (c + 1)
        ].astype(F32)


def local_edge(fetch_ref, edge, spare):
    return jnp.minimum(fetch_ref[edge].astype(jnp.uint32), jnp.uint32(spare)).astype(jnp.int32)


def for_slots(send_ref, step):
    directions, _, each = send_ref.shape

    def body(t, carry):
        for r in range(each):
            step(t, r, t * each + r)
        return carry

    lax.fori_loop(0, directions, body, 0)


def pack_kernel(
    send_hbm_ref,
    rows_hbm_ref,
    low_ref,
    middle_ref,
    high_ref,
    send_ref,
    rows_ref,
    wide_ref,
    packed_ref,
    copied,
    listed,
):
    count = rows_ref.shape[0]
    each = send_ref.shape[2]
    chunk = count // 8
    copies = [
        pltpu.make_async_copy(
            rows_hbm_ref.at[pl.ds(chunk * i, chunk), :],
            rows_ref.at[pl.ds(chunk * i, chunk), :],
            copied.at[i],
        )
        for i in range(8)
    ]
    slots = pltpu.make_async_copy(send_hbm_ref, send_ref, listed)
    slots.start()
    wide_ref[0:32, :] = jnp.zeros((32, 128), F32)
    for copy in copies:
        copy.start()
    for i, copy in enumerate(copies):
        copy.wait()
        spread_rows(rows_ref, wide_ref, chunk * i, chunk, 8)
    slots.wait()

    def pick(t, r, s):
        source = pl.multiple_of(send_ref[t, 0, r] * 4 + 32, 4)
        packed_ref[pl.ds(pl.multiple_of(s * 4, 4), 4), :] = wide_ref[pl.ds(source, 4), :]

    for_slots(send_ref, pick)
    slab = 9 * 4 * each
    for i, out_ref in enumerate((low_ref, middle_ref, high_ref)):
        out_ref[...] = packed_ref[slab * i : slab * (i + 1), :].astype(BF16)


def local_kernel(fetch_ref, rows_ref, out_ref, wide_ref):
    count = rows_ref.shape[0]
    for start in range(0, count, 256):
        spread_rows(rows_ref, wide_ref, start, 256)
    wide_ref[4 * count : 4 * count + 8, :] = jnp.zeros((8, 128), F32)
    unroll = 32

    def body(i, carry):
        for k in range(unroll):
            source = pl.multiple_of(local_edge(fetch_ref, i * unroll + k, count) * 4, 4)
            target = pl.multiple_of((i * unroll + k) * 4, 4)
            out_ref[pl.ds(target, 4), :] = wide_ref[pl.ds(source, 4), :]
        return carry

    lax.fori_loop(0, count // unroll, body, 0)


def widen_arrived(pieces, wide_ref):
    for c, piece in enumerate(pieces):
        rows = piece.shape[0] // 9
        for i in range(9):
            start = rows * (9 * (i % 3) + 3 * (i // 3) + c)
            wide_ref[start : start + rows, :] = piece[rows * i : rows * (i + 1), :].astype(F32)


def blocks_kernel(
    send_ref,
    low_ref,
    middle_ref,
    high_ref,
    reverse_ref,
    weight_ref,
    bins_ref,
    down_ref,
    mixer_ref,
    up_ref,
    first_ref,
    second_ref,
    trip_ref,
    send_low_ref,
    send_middle_ref,
    send_high_ref,
    arrived32_ref,
    rows_ref,
    wide_ref,
    summed_ref,
    packed_ref,
    mixed_ref,
    inner_ref,
):
    count = rows_ref.shape[0]
    groups = summed_ref.shape[0] // 32
    trip = up_ref.shape[1]
    angular = summed_ref.shape[1] // 256
    widen_arrived((low_ref, middle_ref, high_ref), arrived32_ref)

    def place(t, r, s):
        target = pl.multiple_of(send_ref[t, 0, r] * 4, 4)
        reverse_ref[pl.ds(target, 4), :] = arrived32_ref[pl.ds(pl.multiple_of(s * 4, 4), 4), :]

    for_slots(send_ref, place)
    for start in range(0, count, 256):
        for c in range(4):
            rows_ref[start : start + 256, 128 * c : 128 * (c + 1)] = reverse_ref[
                pl.ds(4 * start + c, 256, stride=4), :
            ].astype(BF16)
    trip_ref[count : count + 8, :] = jnp.zeros((8, 128), F32)
    step = 256
    shape = (step, 4 * trip)
    own_lanes = (
        lax.broadcasted_iota(jnp.int32, shape, 0) // 32 % 4
        == lax.broadcasted_iota(jnp.int32, shape, 1) // trip
    )
    downs = [jnp.concatenate([down_ref[block]] * 4, axis=0) for block in range(2)]

    def project(i, block):
        at = span(i, step)
        projected = silu_of_half(dot_t(rows_ref[at, :], downs[block]))
        wide_ref[at, :] = jnp.where(own_lanes, projected, 0.0).astype(BF16)

    def lift(i):
        at = span(i, step)
        lifted = silu_of_half(dot(trip_ref[at, :trip].astype(BF16), up_ref[0]))
        rows = rows_ref[at, :].astype(F32)
        mixed_ref[at, :] = ((rows + lifted) * HALF_ROOT).astype(BF16)

    def first(i):
        at = span(i, step)
        inner_ref[at, :] = silu_of_half(dot(mixed_ref[at, :], first_ref[0])).astype(BF16)

    def second(i):
        at = span(i, step)
        change = silu_of_half(dot(inner_ref[at, :], second_ref[0]))
        rows_ref[at, :] = ((mixed_ref[at, :].astype(F32) + change) * HALF_ROOT).astype(BF16)

    def group(g, carry):
        start = pl.multiple_of(g * 32, 32)
        weight = weight_ref[pl.ds(start, 32), :]
        bins = bins_ref[pl.ds(start, 32), :]
        zero = jnp.zeros_like(weight)
        chosen = [jnp.where(bins == b, weight, zero) for b in range(angular)]
        own = wide_ref[pl.ds(pl.multiple_of(g * 128, 128), 128), :]
        sums = dot(jnp.concatenate(chosen, axis=0), own).astype(BF16)
        for b in range(angular):
            summed_ref[pl.ds(start, 32), 256 * b : 256 * (b + 1)] = sums[32 * b : 32 * (b + 1), :]
        return carry

    for i in range(count // step):
        project(i, 0)
    for block in range(2):
        lax.fori_loop(0, groups, group, 0, unroll=8)
        triplet = dot(summed_ref[...], mixer_ref[block]).astype(BF16).astype(F32)
        for g in range(groups):
            for a in range(4):
                start = 128 * g + 32 * a
                trip_ref[start : start + 32, trip * block : trip * (block + 1)] = triplet[
                    32 * g : 32 * (g + 1), trip * a : trip * (a + 1)
                ]
        if block == 0:
            pipelined(count // step, (lift, first, second, lambda i: project(i, 1)), BLOCK_TRIPS)

    def pick(t, r, s):
        packed_ref[pl.ds(s, 1), :] = trip_ref[pl.ds(send_ref[t, 0, r], 1), :]

    for_slots(send_ref, pick)
    slab = packed_ref.shape[0] // 3
    for i, out_ref in enumerate((send_low_ref, send_middle_ref, send_high_ref)):
        out_ref[...] = packed_ref[slab * i : slab * (i + 1), :].astype(BF16)


def trip_kernel(fetch_ref, trip_ref, out_ref):
    count = fetch_ref.shape[0]
    unroll = 32

    def body(i, carry):
        for k in range(unroll):
            edge = i * unroll + k
            out_ref[pl.ds(edge, 1), :] = trip_ref[pl.ds(local_edge(fetch_ref, edge, count), 1), :]
        return carry

    lax.fori_loop(0, count // unroll, body, 0)


def final_kernel(
    send_ref,
    low_ref,
    middle_ref,
    high_ref,
    trip_ref,
    rows_ref,
    live_ref,
    up_ref,
    first_ref,
    second_ref,
    out_ref,
    arrived32_ref,
    mixed_ref,
    inner_ref,
    mixed_next_ref,
    inner_next_ref,
    rows_out_ref,
    mask_ref,
    copied,
):
    count = rows_ref.shape[0]
    trip = up_ref.shape[1]
    widen_arrived((low_ref, middle_ref, high_ref), arrived32_ref)

    def place(t, r, s):
        trip_ref[pl.ds(send_ref[t, 0, r], 1), :] = arrived32_ref[pl.ds(s, 1), :]

    for_slots(send_ref, place)
    step = 256

    def lifted(at, block):
        both = trip_ref[at, :].astype(BF16)
        return silu_of_half(dot(both[:, trip * block : trip * (block + 1)], up_ref[block]))

    def lift(i):
        at = span(i, step)
        for h in range(step // 128):
            g = i * (step // 128) + h
            line = live_ref[pl.ds(g, 1), :].astype(F32)
            mask_ref[span(g, 128), :] = jnp.broadcast_to(line, (128, 128)).T
        rows = rows_ref[at, :].astype(F32)
        mixed_ref[at, :] = ((rows + lifted(at, 0)) * HALF_ROOT).astype(BF16)

    def first(i):
        at = span(i, step)
        inner_ref[at, :] = silu_of_half(dot(mixed_ref[at, :], first_ref[0])).astype(BF16)

    def second(i):
        at = span(i, step)
        change = silu_of_half(dot(inner_ref[at, :], second_ref[0]))
        rows = (mixed_ref[at, :].astype(F32) + change) * HALF_ROOT
        mixed_next_ref[at, :] = ((rows + lifted(at, 1)) * HALF_ROOT).astype(BF16)

    def first_next(i):
        at = span(i, step)
        inner_next_ref[at, :] = silu_of_half(dot(mixed_next_ref[at, :], first_ref[1])).astype(BF16)

    def second_next(i):
        at = span(i, step)
        change = silu_of_half(dot(inner_next_ref[at, :], second_ref[1]))
        rows = (mixed_next_ref[at, :].astype(F32) + change) * HALF_ROOT
        for c in range(4):
            lanes = slice(128 * c, 128 * (c + 1))
            rows_out_ref[at, lanes] = jnp.where(mask_ref[at, :] >= 0.0, rows[:, lanes], 0.0).astype(
                BF16
            )
        copy_out(i).start()

    def copy_out(i):
        at = span(i, step)
        return pltpu.make_async_copy(rows_out_ref.at[at, :], out_ref.at[at, :], copied.at[i])

    pipelined(count // step, (lift, first, second, first_next, second_next), FINAL_TRIPS)
    for i in range(count // step):
        copy_out(i).wait()


def prepare_kernel(
    weight_ref,
    bins_ref,
    live_ref,
    bilinear_ref,
    up_ref,
    first_ref,
    second_ref,
    down_ref,
    senders_ref,
    weight_out_ref,
    bins_out_ref,
    mixer_ref,
    up_out_ref,
    first_out_ref,
    second_out_ref,
    down_out_ref,
    slots_ref,
):
    count = weight_ref.shape[1]
    slots_ref[...] = jnp.where(senders_ref[...] < 0, count, senders_ref[...])
    neigh = weight_ref.shape[0]
    side = 4 * neigh
    groups = weight_ref.shape[1] // side
    trip = bilinear_ref.shape[1]
    angular = bilinear_ref.shape[2] // trip
    row = lax.broadcasted_iota(jnp.int32, (side, side), 0)
    lane = lax.broadcasted_iota(jnp.int32, (side, side), 1)
    distinct = row % neigh != lane % neigh
    piece = lax.broadcasted_iota(jnp.int32, (neigh, side), 1) // neigh

    def turn(blocks):
        stacked = []
        for a in range(4):
            rows = jnp.zeros((neigh, side), F32)
            for h in range(4):
                shift = (h - a) * neigh % side
                moved = pltpu.roll(blocks[h], shift, 1) if shift else blocks[h]
                rows = jnp.where(piece == h, moved, rows)
            stacked.append(rows)
        return jnp.concatenate(stacked, axis=0).T

    for start in range(0, groups, 4):
        spans = [slice(side * (start + h), side * (start + h + 1)) for h in range(4)]
        rows = slice(neigh * start, neigh * start + side)
        weight_out_ref[rows, :] = turn([weight_ref[:, span] for span in spans]).astype(BF16)
        live = jnp.concatenate(
            [
                jnp.broadcast_to(live_ref[start + h : start + h + 1, :], (neigh, side))
                for h in range(4)
            ],
            axis=0,
        )
        bins = turn([bins_ref[:, span].astype(F32) for span in spans])
        bins_out_ref[rows, :] = jnp.where(distinct & (live >= 0), bins, -1.0).astype(BF16)
    lane_block = lax.broadcasted_iota(jnp.int32, (trip, 4 * trip), 1) // trip
    for block in range(2):
        turned = bilinear_ref[block].astype(F32).T
        wide = jnp.concatenate([turned] * 4, axis=1)
        for b in range(angular):
            part = wide[trip * b : trip * (b + 1), :]
            for a in range(4):
                start = 4 * trip * b + trip * a
                mixer_ref[block, start : start + trip, :] = jnp.where(
                    lane_block == a, part, 0.0
                ).astype(BF16)
    for source, target in (
        (up_ref, up_out_ref),
        (first_ref, first_out_ref),
        (second_ref, second_out_ref),
        (down_ref, down_out_ref),
    ):
        target[...] = (source[...].astype(F32) * 0.5).astype(BF16)


def local(
    edge_state,
    angle_weight,
    angle_bins,
    send_slots,
    fetch_index,
    down_weight,
    bilinear,
    up_weight,
    first_dense,
    second_dense,
):
    count, width = edge_state.shape
    neigh = angle_weight.shape[1]
    trip = down_weight.shape[2]
    angular = bilinear.shape[1] // trip
    slots = 27 * send_slots.shape[-1]
    quarter = count // 4
    groups = count // (4 * neigh)
    spare = count + 8
    live_lines = fetch_index.reshape(groups, 4 * neigh)
    each = send_slots.shape[-1]
    senders = send_slots.reshape(27, 1, each)
    down_turned = jnp.swapaxes(down_weight, 1, 2)

    smem = pl.BlockSpec(memory_space=pltpu.SMEM)
    vmem = pl.BlockSpec(memory_space=pltpu.VMEM)

    def params(mib):
        return pltpu.CompilerParams(vmem_limit_bytes=mib * MIB)

    outside = pl.BlockSpec(memory_space=pltpu.HBM)
    slab = slots // 3
    packed = pl.pallas_call(
        pack_kernel,
        out_shape=(jax.ShapeDtypeStruct((slab * 4, 128), BF16),) * 3,
        in_specs=[outside, outside],
        out_specs=(vmem,) * 3,
        scratch_shapes=[
            pltpu.SMEM((27, 1, each), jnp.int32),
            pltpu.VMEM((count, width), BF16),
            pltpu.VMEM((spare * 4, 128), F32),
            pltpu.VMEM((slots * 4, 128), F32),
            pltpu.SemaphoreType.DMA((8,)),
            pltpu.SemaphoreType.DMA,
        ],
        compiler_params=params(14),
        name="pack",
    )(
        pltpu.with_memory_space_constraint(senders, pltpu.HBM),
        pltpu.with_memory_space_constraint(edge_state, pltpu.HBM),
    )
    weights, bins, mixer, up_half, first_half, second_half, down_half, own_slots = pl.pallas_call(
        prepare_kernel,
        out_shape=(
            jax.ShapeDtypeStruct((quarter, 4 * neigh), BF16),
            jax.ShapeDtypeStruct((quarter, 4 * neigh), BF16),
            jax.ShapeDtypeStruct((2, angular * 4 * trip, 4 * trip), BF16),
            jax.ShapeDtypeStruct(up_weight.shape, BF16),
            jax.ShapeDtypeStruct(first_dense.shape, BF16),
            jax.ShapeDtypeStruct(second_dense.shape, BF16),
            jax.ShapeDtypeStruct(down_turned.shape, BF16),
            jax.ShapeDtypeStruct(senders.shape, jnp.int32),
        ),
        in_specs=[vmem] * 9,
        out_specs=(vmem,) * 8,
        compiler_params=params(16),
        name="prepare",
    )(
        angle_weight.T,
        angle_bins.T,
        live_lines,
        jnp.swapaxes(bilinear, 1, 2),
        up_weight,
        first_dense,
        second_dense,
        down_turned,
        senders,
    )
    arrived = exchange(packed)

    reverse = pl.pallas_call(
        local_kernel,
        out_shape=jax.ShapeDtypeStruct((spare * 4, 128), F32),
        in_specs=[smem, vmem],
        out_specs=vmem,
        scratch_shapes=[pltpu.VMEM((spare * 4, 128), F32)],
        compiler_params=params(14),
        name="reverse_local",
    )(fetch_index, edge_state)

    triplet, *sending = pl.pallas_call(
        blocks_kernel,
        out_shape=(
            jax.ShapeDtypeStruct((spare, 2 * trip), F32),
        )
        + (jax.ShapeDtypeStruct((slab, 2 * trip), BF16),) * 3,
        in_specs=[smem] + [vmem] * 11,
        out_specs=(vmem,) * 4,
        scratch_shapes=[
            pltpu.VMEM((slots * 4, 128), F32),
            pltpu.VMEM((count, width), BF16),
            pltpu.VMEM((count, 4 * trip), BF16),
            pltpu.VMEM((quarter, angular * 4 * trip), BF16),
            pltpu.VMEM((slots, 2 * trip), F32),
            pltpu.VMEM((count, width), BF16),
            pltpu.VMEM((count, width), BF16),
        ],
        compiler_params=params(32),
        name="blocks",
    )(
        own_slots,
        *arrived,
        reverse,
        weights,
        bins,
        down_half,
        mixer,
        up_half,
        first_half,
        second_half,
    )
    own_trip = pl.pallas_call(
        trip_kernel,
        out_shape=jax.ShapeDtypeStruct((spare, 2 * trip), F32),
        in_specs=[smem, vmem],
        out_specs=vmem,
        compiler_params=params(5),
        name="trip_local",
    )(fetch_index, triplet)
    carried = exchange(sending)

    out = pl.pallas_call(
        final_kernel,
        out_shape=jax.ShapeDtypeStruct((count, width), BF16),
        in_specs=[smem] + [vmem] * 9,
        out_specs=outside,
        scratch_shapes=[pltpu.VMEM((slots, 2 * trip), F32)]
        + [pltpu.VMEM((count, width), BF16)] * 5
        + [pltpu.VMEM((count, 128), F32)]
        + [pltpu.SemaphoreType.DMA((8,))],
        compiler_params=params(24),
        name="final",
    )(
        own_slots,
        *carried,
        own_trip,
        edge_state,
        live_lines,
        up_half,
        first_half,
        second_half,
    )
    return out


def solution(mesh):
    spread = P(("gx", "gy", "gz"), None)
    in_specs = (
        spread,
        spread,
        spread,
        P("gx", "gy", "gz", None, None),
        P(("gx", "gy", "gz")),
        P(),
        P(),
        P(),
        P(),
        P(),
    )

    return jax.shard_map(local, mesh=mesh, in_specs=in_specs, out_specs=spread, check_vma=False)
```

```python
import jax
import jax.numpy as jnp
from jax import lax
from jax.experimental import pallas as pl
from jax.experimental.pallas import tpu as pltpu
from jax.sharding import PartitionSpec as P


HALF_ROOT = 0.7071067811865476
F32 = jnp.float32
BF16 = jnp.bfloat16
MIB = 1024 * 1024
BLOCK_TRIPS = 2
FINAL_TRIPS = 1


def silu_of_half(half):
    return half + half * jnp.tanh(half)


def dot(a, b):
    return jnp.dot(a, b, preferred_element_type=F32)


def dot_t(a, b):
    return lax.dot_general(a, b, (((1,), (1,)), ((), ())), preferred_element_type=F32)


def from_behind(array, axis, by):
    length = lax.axis_size(axis)
    return lax.ppermute(array, axis, [(i, (i + by) % length) for i in range(length)])


def second_kernel(low_ref, middle_ref, high_ref, *out_refs):
    third = low_ref.shape[0] // 3
    for a, slab_ref in enumerate((low_ref, middle_ref, high_ref)):
        for b, out_ref in enumerate(out_refs):
            out_ref[third * a : third * (a + 1), :] = slab_ref[third * b : third * (b + 1), :]


def third_kernel(low_ref, middle_ref, high_ref, *out_refs):
    rows = low_ref.shape[0] // 9
    for b, slab_ref in enumerate((low_ref, middle_ref, high_ref)):
        for a in range(3):
            for c, out_ref in enumerate(out_refs):
                source, target = rows * (3 * a + c), rows * (3 * b + a)
                out_ref[target : target + rows, :] = slab_ref[source : source + rows, :]


def exchange(slabs):
    vmem = pl.BlockSpec(memory_space=pltpu.VMEM)

    def regroup(kernel, pieces):
        return pl.pallas_call(
            kernel,
            out_shape=[jax.ShapeDtypeStruct(piece.shape, piece.dtype) for piece in pieces],
            in_specs=[vmem] * 3,
            out_specs=[vmem] * 3,
            compiler_params=pltpu.CompilerParams(vmem_limit_bytes=4 * MIB),
            name="regroup",
        )(*pieces)

    def hop(sent, axis):
        low, middle, high = sent
        return [from_behind(high, axis, 1), middle, from_behind(low, axis, -1)]

    slabs = hop(slabs, "gx")
    slabs = hop(regroup(second_kernel, slabs), "gy")
    return hop(regroup(third_kernel, slabs), "gz")


def pipelined(blocks, stages, trips):
    share = blocks // trips

    def trip(t, carry):
        for step in range(share + len(stages) - 1):
            for depth in reversed(range(len(stages))):
                if 0 <= step - depth < share:
                    stages[depth](t * share + step - depth)
        return carry

    if trips == 1:
        trip(0, 0)
    else:
        lax.fori_loop(0, trips, trip, 0)


def span(i, size):
    if isinstance(i, int):
        return slice(size * i, size * (i + 1))
    return pl.ds(pl.multiple_of(size * i, size), size)


def spread_rows(rows_ref, wide_ref, start, count, shift=0):
    for c in range(4):
        wide_ref[pl.ds(4 * (start + shift) + c, count, stride=4), :] = rows_ref[
            start : start + count, 128 * c : 128 * (c + 1)
        ].astype(F32)


def local_edge(fetch_ref, edge, spare):
    return jnp.minimum(fetch_ref[edge].astype(jnp.uint32), jnp.uint32(spare)).astype(jnp.int32)


def for_slots(send_ref, step, thirds=(0, 1, 2)):
    directions, _, each = send_ref.shape

    def body(i, carry):
        for c in thirds:
            t = 3 * i + c
            for r in range(each):
                step(t, r, t * each + r)
        return carry

    lax.fori_loop(0, directions // 3, body, 0)


def pack_kernel(
    send_hbm_ref,
    rows_hbm_ref,
    low_ref,
    middle_ref,
    high_ref,
    send_ref,
    rows_ref,
    wide_ref,
    packed_ref,
    copied,
    listed,
):
    count = rows_ref.shape[0]
    each = send_ref.shape[2]
    chunk = count // 8
    copies = [
        pltpu.make_async_copy(
            rows_hbm_ref.at[pl.ds(chunk * i, chunk), :],
            rows_ref.at[pl.ds(chunk * i, chunk), :],
            copied.at[i],
        )
        for i in range(8)
    ]
    slots = pltpu.make_async_copy(send_hbm_ref, send_ref, listed)
    slots.start()
    wide_ref[0:32, :] = jnp.zeros((32, 128), F32)
    for copy in copies:
        copy.start()
    for i, copy in enumerate(copies):
        copy.wait()
        spread_rows(rows_ref, wide_ref, chunk * i, chunk, 8)
    slots.wait()

    def pick(t, r, s):
        source = pl.multiple_of(send_ref[t, 0, r] * 4 + 32, 4)
        packed_ref[pl.ds(pl.multiple_of(s * 4, 4), 4), :] = wide_ref[pl.ds(source, 4), :]

    for_slots(send_ref, pick)
    slab = 9 * 4 * each
    for i, out_ref in enumerate((low_ref, middle_ref, high_ref)):
        out_ref[...] = packed_ref[slab * i : slab * (i + 1), :].astype(BF16)


def place_wide(send_ref, arrived_ref, rows_ref, t, r, s):
    target = pl.multiple_of(send_ref[t, 0, r] * 4, 4)
    rows_ref[pl.ds(target, 4), :] = arrived_ref[pl.ds(pl.multiple_of(s * 4, 4), 4), :]


def local_kernel(fetch_ref, send_ref, middle_ref, rows_ref, out_ref, wide_ref, arrived32_ref):
    count = rows_ref.shape[0]
    for start in range(0, count, 256):
        spread_rows(rows_ref, wide_ref, start, 256)
    wide_ref[4 * count : 4 * count + 8, :] = jnp.zeros((8, 128), F32)
    unroll = 32

    def body(i, carry):
        for k in range(unroll):
            source = pl.multiple_of(local_edge(fetch_ref, i * unroll + k, count) * 4, 4)
            target = pl.multiple_of((i * unroll + k) * 4, 4)
            out_ref[pl.ds(target, 4), :] = wide_ref[pl.ds(source, 4), :]
        return carry

    lax.fori_loop(0, count // unroll, body, 0)
    widen_arrived(((1, middle_ref),), arrived32_ref)
    for_slots(send_ref, lambda t, r, s: place_wide(send_ref, arrived32_ref, out_ref, t, r, s), (1,))


def widen_arrived(pieces, wide_ref):
    for c, piece in pieces:
        rows = piece.shape[0] // 9
        for i in range(9):
            start = rows * (9 * (i % 3) + 3 * (i // 3) + c)
            wide_ref[start : start + rows, :] = piece[rows * i : rows * (i + 1), :].astype(F32)


def blocks_kernel(
    send_hbm_ref,
    low_ref,
    high_ref,
    reverse_ref,
    weight_ref,
    bins_ref,
    down_ref,
    mixer_ref,
    up_ref,
    first_ref,
    second_ref,
    trip_ref,
    send_low_ref,
    send_middle_ref,
    send_high_ref,
    arrived32_ref,
    rows_ref,
    wide_ref,
    summed_ref,
    packed_ref,
    mixed_ref,
    inner_ref,
    send_ref,
    listed,
):
    count = rows_ref.shape[0]
    groups = summed_ref.shape[0] // 32
    trip = up_ref.shape[1]
    angular = summed_ref.shape[1] // 256
    listing = pltpu.make_async_copy(send_hbm_ref, send_ref, listed)
    listing.start()
    widen_arrived(((0, low_ref), (2, high_ref)), arrived32_ref)
    listing.wait()
    for_slots(
        send_ref,
        lambda t, r, s: place_wide(send_ref, arrived32_ref, reverse_ref, t, r, s),
        (0, 2),
    )
    for start in range(0, count, 256):
        for c in range(4):
            rows_ref[start : start + 256, 128 * c : 128 * (c + 1)] = reverse_ref[
                pl.ds(4 * start + c, 256, stride=4), :
            ].astype(BF16)
    trip_ref[count : count + 8, :] = jnp.zeros((8, 128), F32)
    step = 256
    shape = (step, 4 * trip)
    own_lanes = (
        lax.broadcasted_iota(jnp.int32, shape, 0) // 32 % 4
        == lax.broadcasted_iota(jnp.int32, shape, 1) // trip
    )
    downs = [jnp.concatenate([down_ref[block]] * 4, axis=0) for block in range(2)]

    def project(i, block):
        at = span(i, step)
        projected = silu_of_half(dot_t(rows_ref[at, :], downs[block]))
        wide_ref[at, :] = jnp.where(own_lanes, projected, 0.0).astype(BF16)

    def lift(i):
        at = span(i, step)
        lifted = silu_of_half(dot(trip_ref[at, :trip].astype(BF16), up_ref[0]))
        rows = rows_ref[at, :].astype(F32)
        mixed_ref[at, :] = ((rows + lifted) * HALF_ROOT).astype(BF16)

    def first(i):
        at = span(i, step)
        inner_ref[at, :] = silu_of_half(dot(mixed_ref[at, :], first_ref[0])).astype(BF16)

    def second(i):
        at = span(i, step)
        change = silu_of_half(dot(inner_ref[at, :], second_ref[0]))
        rows_ref[at, :] = ((mixed_ref[at, :].astype(F32) + change) * HALF_ROOT).astype(BF16)

    def group(g, carry):
        start = pl.multiple_of(g * 32, 32)
        weight = weight_ref[pl.ds(start, 32), :]
        bins = bins_ref[pl.ds(start, 32), :]
        zero = jnp.zeros_like(weight)
        chosen = [jnp.where(bins == b, weight, zero) for b in range(angular)]
        own = wide_ref[pl.ds(pl.multiple_of(g * 128, 128), 128), :]
        sums = dot(jnp.concatenate(chosen, axis=0), own).astype(BF16)
        for b in range(angular):
            summed_ref[pl.ds(start, 32), 256 * b : 256 * (b + 1)] = sums[32 * b : 32 * (b + 1), :]
        return carry

    for i in range(count // step):
        project(i, 0)
    for block in range(2):
        lax.fori_loop(0, groups, group, 0, unroll=8)
        triplet = dot(summed_ref[...], mixer_ref[block]).astype(BF16).astype(F32)
        for g in range(groups):
            for a in range(4):
                start = 128 * g + 32 * a
                trip_ref[start : start + 32, trip * block : trip * (block + 1)] = triplet[
                    32 * g : 32 * (g + 1), trip * a : trip * (a + 1)
                ]
        if block == 0:
            pipelined(count // step, (lift, first, second, lambda i: project(i, 1)), BLOCK_TRIPS)

    def pick(t, r, s):
        packed_ref[pl.ds(s, 1), :] = trip_ref[pl.ds(send_ref[t, 0, r], 1), :]

    for_slots(send_ref, pick)
    slab = packed_ref.shape[0] // 3
    for i, out_ref in enumerate((send_low_ref, send_middle_ref, send_high_ref)):
        out_ref[...] = packed_ref[slab * i : slab * (i + 1), :].astype(BF16)


def gather_trips(fetch_ref, trip_ref, out_ref, start, count, spare):
    unroll = 32

    def body(i, carry):
        for k in range(unroll):
            edge = start + i * unroll + k
            out_ref[pl.ds(edge, 1), :] = trip_ref[pl.ds(local_edge(fetch_ref, edge, spare), 1), :]
        return carry

    lax.fori_loop(0, count // unroll, body, 0)


def trip_kernel(fetch_ref, trip_ref, out_ref):
    gather_trips(fetch_ref, trip_ref, out_ref, 0, out_ref.shape[0], fetch_ref.shape[0])


def trip_rest_kernel(fetch_ref, trip_ref, begun_ref, out_ref):
    count = fetch_ref.shape[0]
    done = begun_ref.shape[0]
    out_ref[0:done, :] = begun_ref[...]
    gather_trips(fetch_ref, trip_ref, out_ref, done, count - done, count)


def trip_middle_kernel(send_ref, middle_ref, begun_ref, out_ref, arrived32_ref):
    out_ref[...] = begun_ref[...]
    widen_arrived(((1, middle_ref),), arrived32_ref)

    def place(t, r, s):
        out_ref[pl.ds(send_ref[t, 0, r], 1), :] = arrived32_ref[pl.ds(s, 1), :]

    for_slots(send_ref, place, (1,))


def final_kernel(
    send_hbm_ref,
    low_ref,
    high_ref,
    trip_ref,
    rows_ref,
    live_ref,
    up_ref,
    first_ref,
    second_ref,
    out_ref,
    arrived32_ref,
    mixed_ref,
    inner_ref,
    mixed_next_ref,
    inner_next_ref,
    rows_out_ref,
    mask_ref,
    copied,
    send_ref,
    listed,
):
    count = rows_ref.shape[0]
    trip = up_ref.shape[1]
    listing = pltpu.make_async_copy(send_hbm_ref, send_ref, listed)
    listing.start()
    widen_arrived(((0, low_ref), (2, high_ref)), arrived32_ref)
    listing.wait()

    def place(t, r, s):
        trip_ref[pl.ds(send_ref[t, 0, r], 1), :] = arrived32_ref[pl.ds(s, 1), :]

    for_slots(send_ref, place, (0, 2))
    step = 256

    def lifted(at, block):
        both = trip_ref[at, :].astype(BF16)
        return silu_of_half(dot(both[:, trip * block : trip * (block + 1)], up_ref[block]))

    def lift(i):
        at = span(i, step)
        for g in range(i * (step // 128), (i + 1) * (step // 128)):
            line = live_ref[g : g + 1, :].astype(F32)
            mask_ref[span(g, 128), :] = jnp.broadcast_to(line, (128, 128)).T
        rows = rows_ref[at, :].astype(F32)
        mixed_ref[at, :] = ((rows + lifted(at, 0)) * HALF_ROOT).astype(BF16)

    def first(i):
        at = span(i, step)
        inner_ref[at, :] = silu_of_half(dot(mixed_ref[at, :], first_ref[0])).astype(BF16)

    def second(i):
        at = span(i, step)
        change = silu_of_half(dot(inner_ref[at, :], second_ref[0]))
        rows = (mixed_ref[at, :].astype(F32) + change) * HALF_ROOT
        mixed_next_ref[at, :] = ((rows + lifted(at, 1)) * HALF_ROOT).astype(BF16)

    def first_next(i):
        at = span(i, step)
        inner_next_ref[at, :] = silu_of_half(dot(mixed_next_ref[at, :], first_ref[1])).astype(BF16)

    def second_next(i):
        at = span(i, step)
        change = silu_of_half(dot(inner_next_ref[at, :], second_ref[1]))
        rows = (mixed_next_ref[at, :].astype(F32) + change) * HALF_ROOT
        for c in range(4):
            lanes = slice(128 * c, 128 * (c + 1))
            rows_out_ref[at, lanes] = jnp.where(mask_ref[at, :] >= 0.0, rows[:, lanes], 0.0).astype(
                BF16
            )
        copy_out(i).start()

    def copy_out(i):
        at = span(i, step)
        return pltpu.make_async_copy(rows_out_ref.at[at, :], out_ref.at[at, :], copied.at[i])

    pipelined(count // step, (lift, first, second, first_next, second_next), FINAL_TRIPS)
    for i in range(count // step):
        copy_out(i).wait()


def prepare_kernel(
    weight_ref,
    bins_ref,
    live_ref,
    bilinear_ref,
    up_ref,
    first_ref,
    second_ref,
    down_ref,
    senders_ref,
    weight_out_ref,
    bins_out_ref,
    mixer_ref,
    up_out_ref,
    first_out_ref,
    second_out_ref,
    down_out_ref,
    slots_ref,
):
    count = weight_ref.shape[1]
    slots_ref[...] = jnp.where(senders_ref[...] < 0, count, senders_ref[...])
    neigh = weight_ref.shape[0]
    side = 4 * neigh
    groups = weight_ref.shape[1] // side
    trip = bilinear_ref.shape[1]
    angular = bilinear_ref.shape[2] // trip
    row = lax.broadcasted_iota(jnp.int32, (side, side), 0)
    lane = lax.broadcasted_iota(jnp.int32, (side, side), 1)
    distinct = row % neigh != lane % neigh
    piece = lax.broadcasted_iota(jnp.int32, (neigh, side), 1) // neigh

    def turn(blocks):
        stacked = []
        for a in range(4):
            rows = jnp.zeros((neigh, side), F32)
            for h in range(4):
                shift = (h - a) * neigh % side
                moved = pltpu.roll(blocks[h], shift, 1) if shift else blocks[h]
                rows = jnp.where(piece == h, moved, rows)
            stacked.append(rows)
        return jnp.concatenate(stacked, axis=0).T

    for start in range(0, groups, 4):
        spans = [slice(side * (start + h), side * (start + h + 1)) for h in range(4)]
        rows = slice(neigh * start, neigh * start + side)
        weight_out_ref[rows, :] = turn([weight_ref[:, span] for span in spans]).astype(BF16)
        live = jnp.concatenate(
            [
                jnp.broadcast_to(live_ref[start + h : start + h + 1, :], (neigh, side))
                for h in range(4)
            ],
            axis=0,
        )
        bins = turn([bins_ref[:, span].astype(F32) for span in spans])
        bins_out_ref[rows, :] = jnp.where(distinct & (live >= 0), bins, -1.0).astype(BF16)
    lane_block = lax.broadcasted_iota(jnp.int32, (trip, 4 * trip), 1) // trip
    for block in range(2):
        turned = bilinear_ref[block].astype(F32).T
        wide = jnp.concatenate([turned] * 4, axis=1)
        for b in range(angular):
            part = wide[trip * b : trip * (b + 1), :]
            for a in range(4):
                start = 4 * trip * b + trip * a
                mixer_ref[block, start : start + trip, :] = jnp.where(
                    lane_block == a, part, 0.0
                ).astype(BF16)
    for source, target in (
        (up_ref, up_out_ref),
        (first_ref, first_out_ref),
        (second_ref, second_out_ref),
        (down_ref, down_out_ref),
    ):
        target[...] = (source[...].astype(F32) * 0.5).astype(BF16)


def local(
    edge_state,
    angle_weight,
    angle_bins,
    send_slots,
    fetch_index,
    down_weight,
    bilinear,
    up_weight,
    first_dense,
    second_dense,
):
    count, width = edge_state.shape
    neigh = angle_weight.shape[1]
    trip = down_weight.shape[2]
    angular = bilinear.shape[1] // trip
    slots = 27 * send_slots.shape[-1]
    quarter = count // 4
    groups = count // (4 * neigh)
    spare = count + 8
    live_lines = fetch_index.reshape(groups, 4 * neigh)
    each = send_slots.shape[-1]
    senders = send_slots.reshape(27, 1, each)
    down_turned = jnp.swapaxes(down_weight, 1, 2)

    smem = pl.BlockSpec(memory_space=pltpu.SMEM)
    vmem = pl.BlockSpec(memory_space=pltpu.VMEM)

    def params(mib):
        return pltpu.CompilerParams(vmem_limit_bytes=mib * MIB)

    outside = pl.BlockSpec(memory_space=pltpu.HBM)
    slab = slots // 3
    packed = pl.pallas_call(
        pack_kernel,
        out_shape=(jax.ShapeDtypeStruct((slab * 4, 128), BF16),) * 3,
        in_specs=[outside, outside],
        out_specs=(vmem,) * 3,
        scratch_shapes=[
            pltpu.SMEM((27, 1, each), jnp.int32),
            pltpu.VMEM((count, width), BF16),
            pltpu.VMEM((spare * 4, 128), F32),
            pltpu.VMEM((slots * 4, 128), F32),
            pltpu.SemaphoreType.DMA((8,)),
            pltpu.SemaphoreType.DMA,
        ],
        compiler_params=params(14),
        name="pack",
    )(
        pltpu.with_memory_space_constraint(senders, pltpu.HBM),
        pltpu.with_memory_space_constraint(edge_state, pltpu.HBM),
    )
    weights, bins, mixer, up_half, first_half, second_half, down_half, own_slots = pl.pallas_call(
        prepare_kernel,
        out_shape=(
            jax.ShapeDtypeStruct((quarter, 4 * neigh), BF16),
            jax.ShapeDtypeStruct((quarter, 4 * neigh), BF16),
            jax.ShapeDtypeStruct((2, angular * 4 * trip, 4 * trip), BF16),
            jax.ShapeDtypeStruct(up_weight.shape, BF16),
            jax.ShapeDtypeStruct(first_dense.shape, BF16),
            jax.ShapeDtypeStruct(second_dense.shape, BF16),
            jax.ShapeDtypeStruct(down_turned.shape, BF16),
            jax.ShapeDtypeStruct(senders.shape, jnp.int32),
        ),
        in_specs=[vmem] * 9,
        out_specs=(vmem,) * 8,
        compiler_params=params(16),
        name="prepare",
    )(
        angle_weight.T,
        angle_bins.T,
        live_lines,
        jnp.swapaxes(bilinear, 1, 2),
        up_weight,
        first_dense,
        second_dense,
        down_turned,
        senders,
    )
    hbm_slots = pltpu.with_memory_space_constraint(own_slots, pltpu.HBM)
    arrived = exchange(packed)

    reverse = pl.pallas_call(
        local_kernel,
        out_shape=jax.ShapeDtypeStruct((spare * 4, 128), F32),
        in_specs=[smem, smem, vmem, vmem],
        out_specs=vmem,
        scratch_shapes=[
            pltpu.VMEM((spare * 4, 128), F32),
            pltpu.VMEM((slots * 4, 128), F32),
        ],
        compiler_params=params(16),
        name="reverse_local",
    )(fetch_index, own_slots, arrived[1], edge_state)

    triplet, *sending = pl.pallas_call(
        blocks_kernel,
        out_shape=(
            jax.ShapeDtypeStruct((spare, 2 * trip), F32),
        )
        + (jax.ShapeDtypeStruct((slab, 2 * trip), BF16),) * 3,
        in_specs=[outside] + [vmem] * 10,
        out_specs=(vmem,) * 4,
        scratch_shapes=[
            pltpu.VMEM((slots * 4, 128), F32),
            pltpu.VMEM((count, width), BF16),
            pltpu.VMEM((count, 4 * trip), BF16),
            pltpu.VMEM((quarter, angular * 4 * trip), BF16),
            pltpu.VMEM((slots, 2 * trip), F32),
            pltpu.VMEM((count, width), BF16),
            pltpu.VMEM((count, width), BF16),
            pltpu.SMEM(senders.shape, jnp.int32),
            pltpu.SemaphoreType.DMA,
        ],
        compiler_params=params(32),
        name="blocks",
    )(
        hbm_slots,
        arrived[0],
        arrived[2],
        reverse,
        weights,
        bins,
        down_half,
        mixer,
        up_half,
        first_half,
        second_half,
    )
    carried = exchange(sending)
    own_trip = pl.pallas_call(
        trip_kernel,
        out_shape=jax.ShapeDtypeStruct((count // 2, 2 * trip), F32),
        in_specs=[smem, vmem],
        out_specs=vmem,
        compiler_params=params(5),
        name="trip_local",
    )(fetch_index, triplet)
    own_trip = pl.pallas_call(
        trip_rest_kernel,
        out_shape=jax.ShapeDtypeStruct((spare, 2 * trip), F32),
        in_specs=[smem, vmem, vmem],
        out_specs=vmem,
        compiler_params=params(5),
        name="trip_rest",
    )(fetch_index, triplet, own_trip)
    own_trip = pl.pallas_call(
        trip_middle_kernel,
        out_shape=jax.ShapeDtypeStruct((spare, 2 * trip), F32),
        in_specs=[smem, vmem, vmem],
        out_specs=vmem,
        scratch_shapes=[pltpu.VMEM((slots, 2 * trip), F32)],
        compiler_params=params(5),
        name="trip_middle",
    )(own_slots, carried[1], own_trip)

    out = pl.pallas_call(
        final_kernel,
        out_shape=jax.ShapeDtypeStruct((count, width), BF16),
        in_specs=[outside] + [vmem] * 8,
        out_specs=outside,
        scratch_shapes=[pltpu.VMEM((slots, 2 * trip), F32)]
        + [pltpu.VMEM((count, width), BF16)] * 5
        + [pltpu.VMEM((count, 128), F32)]
        + [
            pltpu.SemaphoreType.DMA((8,)),
            pltpu.SMEM(senders.shape, jnp.int32),
            pltpu.SemaphoreType.DMA,
        ],
        compiler_params=params(24),
        name="final",
    )(
        hbm_slots,
        carried[0],
        carried[2],
        own_trip,
        edge_state,
        live_lines,
        up_half,
        first_half,
        second_half,
    )
    return out


def solution(mesh):
    spread = P(("gx", "gy", "gz"), None)
    in_specs = (
        spread,
        spread,
        spread,
        P("gx", "gy", "gz", None, None),
        P(("gx", "gy", "gz")),
        P(),
        P(),
        P(),
        P(),
        P(),
    )

    return jax.shard_map(local, mesh=mesh, in_specs=in_specs, out_specs=spread, check_vma=False)
```

```python
import jax
import jax.numpy as jnp
from jax import lax
from jax.experimental import pallas as pl
from jax.experimental.pallas import tpu as pltpu
from jax.sharding import PartitionSpec as P


HALF_ROOT = 0.7071067811865476
F32 = jnp.float32
BF16 = jnp.bfloat16
MIB = 1024 * 1024
BLOCK_TRIPS = 2
FINAL_TRIPS = 1


def silu_of_half(half):
    return half + half * jnp.tanh(half)


def dot(a, b):
    return jnp.dot(a, b, preferred_element_type=F32)


def dot_t(a, b):
    return lax.dot_general(a, b, (((1,), (1,)), ((), ())), preferred_element_type=F32)


def from_behind(array, axis, by):
    length = lax.axis_size(axis)
    return lax.ppermute(array, axis, [(i, (i + by) % length) for i in range(length)])


def second_kernel(low_ref, middle_ref, high_ref, *out_refs):
    third = low_ref.shape[0] // 3
    for a, slab_ref in enumerate((low_ref, middle_ref, high_ref)):
        for b, out_ref in enumerate(out_refs):
            out_ref[third * a : third * (a + 1), :] = slab_ref[third * b : third * (b + 1), :]


def third_kernel(low_ref, middle_ref, high_ref, *out_refs):
    rows = low_ref.shape[0] // 9
    for b, slab_ref in enumerate((low_ref, middle_ref, high_ref)):
        for a in range(3):
            for c, out_ref in enumerate(out_refs):
                source, target = rows * (3 * a + c), rows * (3 * b + a)
                out_ref[target : target + rows, :] = slab_ref[source : source + rows, :]


def exchange(slabs):
    vmem = pl.BlockSpec(memory_space=pltpu.VMEM)

    def regroup(kernel, pieces):
        return pl.pallas_call(
            kernel,
            out_shape=[jax.ShapeDtypeStruct(piece.shape, piece.dtype) for piece in pieces],
            in_specs=[vmem] * 3,
            out_specs=[vmem] * 3,
            compiler_params=pltpu.CompilerParams(vmem_limit_bytes=4 * MIB),
            name="regroup",
        )(*pieces)

    def hop(sent, axis):
        low, middle, high = sent
        return [from_behind(high, axis, 1), middle, from_behind(low, axis, -1)]

    slabs = hop(slabs, "gx")
    slabs = hop(regroup(second_kernel, slabs), "gy")
    return hop(regroup(third_kernel, slabs), "gz")


def pipelined(blocks, stages, trips):
    share = blocks // trips

    def trip(t, carry):
        for step in range(share + len(stages) - 1):
            for depth in reversed(range(len(stages))):
                if 0 <= step - depth < share:
                    stages[depth](t * share + step - depth)
        return carry

    if trips == 1:
        trip(0, 0)
    else:
        lax.fori_loop(0, trips, trip, 0)


def span(i, size):
    if isinstance(i, int):
        return slice(size * i, size * (i + 1))
    return pl.ds(pl.multiple_of(size * i, size), size)


def spread_rows(rows_ref, wide_ref, start, count, shift=0):
    for c in range(4):
        wide_ref[pl.ds(4 * (start + shift) + c, count, stride=4), :] = rows_ref[
            start : start + count, 128 * c : 128 * (c + 1)
        ].astype(F32)


def local_edge(fetch_ref, edge, spare):
    return jnp.minimum(fetch_ref[edge].astype(jnp.uint32), jnp.uint32(spare)).astype(jnp.int32)


def for_slots(send_ref, step, thirds=(0, 1, 2)):
    directions, _, each = send_ref.shape

    def body(i, carry):
        for c in thirds:
            t = 3 * i + c
            for r in range(each):
                step(t, r, t * each + r)
        return carry

    lax.fori_loop(0, directions // 3, body, 0)


def pack_slab(send_ref, wide_ref, packed_ref, out_ref, first):
    each = send_ref.shape[2]

    def body(i, carry):
        for r in range(each):
            source = pl.multiple_of(send_ref[first + i, 0, r] * 4 + 32, 4)
            target = pl.multiple_of((i * each + r) * 4, 4)
            packed_ref[pl.ds(target, 4), :] = wide_ref[pl.ds(source, 4), :]
        return carry

    lax.fori_loop(0, 9, body, 0)
    out_ref[...] = packed_ref[...].astype(BF16)


def pack_kernel(
    send_hbm_ref,
    rows_hbm_ref,
    low_ref,
    high_ref,
    wide_ref,
    send_ref,
    rows_ref,
    packed_low_ref,
    packed_high_ref,
    copied,
    listed,
):
    count = rows_ref.shape[0]
    chunk = count // 8
    copies = [
        pltpu.make_async_copy(
            rows_hbm_ref.at[pl.ds(chunk * i, chunk), :],
            rows_ref.at[pl.ds(chunk * i, chunk), :],
            copied.at[i],
        )
        for i in range(8)
    ]
    slots = pltpu.make_async_copy(send_hbm_ref, send_ref, listed)
    slots.start()
    wide_ref[0:32, :] = jnp.zeros((32, 128), F32)
    wide_ref[4 * count + 32 : 4 * count + 64, :] = jnp.zeros((32, 128), F32)
    for copy in copies:
        copy.start()
    for i, copy in enumerate(copies):
        copy.wait()
        spread_rows(rows_ref, wide_ref, chunk * i, chunk, 8)
    slots.wait()
    pack_slab(send_ref, wide_ref, packed_low_ref, low_ref, 0)
    pack_slab(send_ref, wide_ref, packed_high_ref, high_ref, 18)


def pack_middle_kernel(send_ref, wide_ref, out_ref, packed_ref):
    pack_slab(send_ref, wide_ref, packed_ref, out_ref, 9)


def place_wide(send_ref, arrived_ref, rows_ref, t, r, s):
    target = pl.multiple_of(send_ref[t, 0, r] * 4, 4)
    rows_ref[pl.ds(target, 4), :] = arrived_ref[pl.ds(pl.multiple_of(s * 4, 4), 4), :]


def local_kernel(fetch_ref, send_ref, middle_ref, wide_ref, out_ref, arrived32_ref):
    count = fetch_ref.shape[0]
    unroll = 32

    def body(i, carry):
        for k in range(unroll):
            edge = i * unroll + k
            source = pl.multiple_of(local_edge(fetch_ref, edge, count) * 4 + 32, 4)
            out_ref[pl.ds(pl.multiple_of(edge * 4, 4), 4), :] = wide_ref[pl.ds(source, 4), :]
        return carry

    lax.fori_loop(0, count // unroll, body, 0)
    widen_arrived(((1, middle_ref),), arrived32_ref)
    for_slots(send_ref, lambda t, r, s: place_wide(send_ref, arrived32_ref, out_ref, t, r, s), (1,))


def widen_arrived(pieces, wide_ref):
    for c, piece in pieces:
        rows = piece.shape[0] // 9
        for i in range(9):
            start = rows * (9 * (i % 3) + 3 * (i // 3) + c)
            wide_ref[start : start + rows, :] = piece[rows * i : rows * (i + 1), :].astype(F32)


def blocks_kernel(
    send_hbm_ref,
    low_ref,
    high_ref,
    reverse_ref,
    weight_ref,
    bins_ref,
    down_ref,
    mixer_ref,
    up_ref,
    first_ref,
    second_ref,
    trip_ref,
    send_low_ref,
    send_middle_ref,
    send_high_ref,
    arrived32_ref,
    rows_ref,
    wide_ref,
    summed_ref,
    packed_ref,
    mixed_ref,
    inner_ref,
    send_ref,
    listed,
):
    count = rows_ref.shape[0]
    groups = summed_ref.shape[0] // 32
    trip = up_ref.shape[1]
    angular = summed_ref.shape[1] // 256
    listing = pltpu.make_async_copy(send_hbm_ref, send_ref, listed)
    listing.start()
    widen_arrived(((0, low_ref), (2, high_ref)), arrived32_ref)
    listing.wait()
    for_slots(
        send_ref,
        lambda t, r, s: place_wide(send_ref, arrived32_ref, reverse_ref, t, r, s),
        (0, 2),
    )
    for start in range(0, count, 256):
        for c in range(4):
            rows_ref[start : start + 256, 128 * c : 128 * (c + 1)] = reverse_ref[
                pl.ds(4 * start + c, 256, stride=4), :
            ].astype(BF16)
    trip_ref[count : count + 8, :] = jnp.zeros((8, 128), F32)
    step = 256
    shape = (step, 4 * trip)
    own_lanes = (
        lax.broadcasted_iota(jnp.int32, shape, 0) // 32 % 4
        == lax.broadcasted_iota(jnp.int32, shape, 1) // trip
    )
    downs = [jnp.concatenate([down_ref[block]] * 4, axis=0) for block in range(2)]

    def project(i, block):
        at = span(i, step)
        projected = silu_of_half(dot_t(rows_ref[at, :], downs[block]))
        wide_ref[at, :] = jnp.where(own_lanes, projected, 0.0).astype(BF16)

    def lift(i):
        at = span(i, step)
        lifted = silu_of_half(dot(trip_ref[at, :trip].astype(BF16), up_ref[0]))
        rows = rows_ref[at, :].astype(F32)
        mixed_ref[at, :] = ((rows + lifted) * HALF_ROOT).astype(BF16)

    def first(i):
        at = span(i, step)
        inner_ref[at, :] = silu_of_half(dot(mixed_ref[at, :], first_ref[0])).astype(BF16)

    def second(i):
        at = span(i, step)
        change = silu_of_half(dot(inner_ref[at, :], second_ref[0]))
        rows_ref[at, :] = ((mixed_ref[at, :].astype(F32) + change) * HALF_ROOT).astype(BF16)

    def group(g, carry):
        start = pl.multiple_of(g * 32, 32)
        weight = weight_ref[pl.ds(start, 32), :]
        bins = bins_ref[pl.ds(start, 32), :]
        zero = jnp.zeros_like(weight)
        chosen = [jnp.where(bins == b, weight, zero) for b in range(angular)]
        own = wide_ref[pl.ds(pl.multiple_of(g * 128, 128), 128), :]
        sums = dot(jnp.concatenate(chosen, axis=0), own).astype(BF16)
        for b in range(angular):
            summed_ref[pl.ds(start, 32), 256 * b : 256 * (b + 1)] = sums[32 * b : 32 * (b + 1), :]
        return carry

    for i in range(count // step):
        project(i, 0)
    for block in range(2):
        lax.fori_loop(0, groups, group, 0, unroll=8)
        triplet = dot(summed_ref[...], mixer_ref[block]).astype(BF16).astype(F32)
        for g in range(groups):
            for a in range(4):
                start = 128 * g + 32 * a
                trip_ref[start : start + 32, trip * block : trip * (block + 1)] = triplet[
                    32 * g : 32 * (g + 1), trip * a : trip * (a + 1)
                ]
        if block == 0:
            pipelined(count // step, (lift, first, second, lambda i: project(i, 1)), BLOCK_TRIPS)

    def pick(t, r, s):
        packed_ref[pl.ds(s, 1), :] = trip_ref[pl.ds(send_ref[t, 0, r], 1), :]

    for_slots(send_ref, pick)
    slab = packed_ref.shape[0] // 3
    for i, out_ref in enumerate((send_low_ref, send_middle_ref, send_high_ref)):
        out_ref[...] = packed_ref[slab * i : slab * (i + 1), :].astype(BF16)


def gather_trips(fetch_ref, trip_ref, out_ref, start, count, spare):
    unroll = 32

    def body(i, carry):
        for k in range(unroll):
            edge = start + i * unroll + k
            out_ref[pl.ds(edge, 1), :] = trip_ref[pl.ds(local_edge(fetch_ref, edge, spare), 1), :]
        return carry

    lax.fori_loop(0, count // unroll, body, 0)


def trip_kernel(fetch_ref, trip_ref, out_ref):
    gather_trips(fetch_ref, trip_ref, out_ref, 0, out_ref.shape[0], fetch_ref.shape[0])


def trip_rest_kernel(fetch_ref, trip_ref, begun_ref, out_ref):
    count = fetch_ref.shape[0]
    done = begun_ref.shape[0]
    out_ref[0:done, :] = begun_ref[...]
    gather_trips(fetch_ref, trip_ref, out_ref, done, count - done, count)


def trip_middle_kernel(send_ref, middle_ref, begun_ref, out_ref, arrived32_ref):
    out_ref[...] = begun_ref[...]
    widen_arrived(((1, middle_ref),), arrived32_ref)

    def place(t, r, s):
        out_ref[pl.ds(send_ref[t, 0, r], 1), :] = arrived32_ref[pl.ds(s, 1), :]

    for_slots(send_ref, place, (1,))


def final_kernel(
    send_hbm_ref,
    low_ref,
    high_ref,
    trip_ref,
    rows_ref,
    live_ref,
    up_ref,
    first_ref,
    second_ref,
    out_ref,
    arrived32_ref,
    mixed_ref,
    inner_ref,
    mixed_next_ref,
    inner_next_ref,
    rows_out_ref,
    mask_ref,
    copied,
    send_ref,
    listed,
):
    count = rows_ref.shape[0]
    trip = up_ref.shape[1]
    listing = pltpu.make_async_copy(send_hbm_ref, send_ref, listed)
    listing.start()
    widen_arrived(((0, low_ref), (2, high_ref)), arrived32_ref)
    listing.wait()

    def place(t, r, s):
        trip_ref[pl.ds(send_ref[t, 0, r], 1), :] = arrived32_ref[pl.ds(s, 1), :]

    for_slots(send_ref, place, (0, 2))
    step = 256

    def lifted(at, block):
        both = trip_ref[at, :].astype(BF16)
        return silu_of_half(dot(both[:, trip * block : trip * (block + 1)], up_ref[block]))

    def lift(i):
        at = span(i, step)
        for g in range(i * (step // 128), (i + 1) * (step // 128)):
            line = live_ref[g : g + 1, :].astype(F32)
            mask_ref[span(g, 128), :] = jnp.broadcast_to(line, (128, 128)).T
        rows = rows_ref[at, :].astype(F32)
        mixed_ref[at, :] = ((rows + lifted(at, 0)) * HALF_ROOT).astype(BF16)

    def first(i):
        at = span(i, step)
        inner_ref[at, :] = silu_of_half(dot(mixed_ref[at, :], first_ref[0])).astype(BF16)

    def second(i):
        at = span(i, step)
        change = silu_of_half(dot(inner_ref[at, :], second_ref[0]))
        rows = (mixed_ref[at, :].astype(F32) + change) * HALF_ROOT
        mixed_next_ref[at, :] = ((rows + lifted(at, 1)) * HALF_ROOT).astype(BF16)

    def first_next(i):
        at = span(i, step)
        inner_next_ref[at, :] = silu_of_half(dot(mixed_next_ref[at, :], first_ref[1])).astype(BF16)

    def second_next(i):
        at = span(i, step)
        change = silu_of_half(dot(inner_next_ref[at, :], second_ref[1]))
        rows = (mixed_next_ref[at, :].astype(F32) + change) * HALF_ROOT
        for c in range(4):
            lanes = slice(128 * c, 128 * (c + 1))
            rows_out_ref[at, lanes] = jnp.where(mask_ref[at, :] >= 0.0, rows[:, lanes], 0.0).astype(
                BF16
            )
        copy_out(i).start()

    def copy_out(i):
        at = span(i, step)
        return pltpu.make_async_copy(rows_out_ref.at[at, :], out_ref.at[at, :], copied.at[i])

    pipelined(count // step, (lift, first, second, first_next, second_next), FINAL_TRIPS)
    for i in range(count // step):
        copy_out(i).wait()


def prepare_kernel(
    weight_ref,
    bins_ref,
    live_ref,
    bilinear_ref,
    up_ref,
    first_ref,
    second_ref,
    down_ref,
    senders_ref,
    weight_out_ref,
    bins_out_ref,
    mixer_ref,
    up_out_ref,
    first_out_ref,
    second_out_ref,
    down_out_ref,
    slots_ref,
):
    count = weight_ref.shape[1]
    slots_ref[...] = jnp.where(senders_ref[...] < 0, count, senders_ref[...])
    neigh = weight_ref.shape[0]
    side = 4 * neigh
    groups = weight_ref.shape[1] // side
    trip = bilinear_ref.shape[1]
    angular = bilinear_ref.shape[2] // trip
    row = lax.broadcasted_iota(jnp.int32, (side, side), 0)
    lane = lax.broadcasted_iota(jnp.int32, (side, side), 1)
    distinct = row % neigh != lane % neigh
    piece = lax.broadcasted_iota(jnp.int32, (neigh, side), 1) // neigh

    def turn(blocks):
        stacked = []
        for a in range(4):
            rows = jnp.zeros((neigh, side), F32)
            for h in range(4):
                shift = (h - a) * neigh % side
                moved = pltpu.roll(blocks[h], shift, 1) if shift else blocks[h]
                rows = jnp.where(piece == h, moved, rows)
            stacked.append(rows)
        return jnp.concatenate(stacked, axis=0).T

    for start in range(0, groups, 4):
        spans = [slice(side * (start + h), side * (start + h + 1)) for h in range(4)]
        rows = slice(neigh * start, neigh * start + side)
        weight_out_ref[rows, :] = turn([weight_ref[:, span] for span in spans]).astype(BF16)
        live = jnp.concatenate(
            [
                jnp.broadcast_to(live_ref[start + h : start + h + 1, :], (neigh, side))
                for h in range(4)
            ],
            axis=0,
        )
        bins = turn([bins_ref[:, span].astype(F32) for span in spans])
        bins_out_ref[rows, :] = jnp.where(distinct & (live >= 0), bins, -1.0).astype(BF16)
    lane_block = lax.broadcasted_iota(jnp.int32, (trip, 4 * trip), 1) // trip
    for block in range(2):
        turned = bilinear_ref[block].astype(F32).T
        wide = jnp.concatenate([turned] * 4, axis=1)
        for b in range(angular):
            part = wide[trip * b : trip * (b + 1), :]
            for a in range(4):
                start = 4 * trip * b + trip * a
                mixer_ref[block, start : start + trip, :] = jnp.where(
                    lane_block == a, part, 0.0
                ).astype(BF16)
    for source, target in (
        (up_ref, up_out_ref),
        (first_ref, first_out_ref),
        (second_ref, second_out_ref),
        (down_ref, down_out_ref),
    ):
        target[...] = (source[...].astype(F32) * 0.5).astype(BF16)


def local(
    edge_state,
    angle_weight,
    angle_bins,
    send_slots,
    fetch_index,
    down_weight,
    bilinear,
    up_weight,
    first_dense,
    second_dense,
):
    count, width = edge_state.shape
    neigh = angle_weight.shape[1]
    trip = down_weight.shape[2]
    angular = bilinear.shape[1] // trip
    slots = 27 * send_slots.shape[-1]
    quarter = count // 4
    groups = count // (4 * neigh)
    spare = count + 8
    live_lines = fetch_index.reshape(groups, 4 * neigh)
    each = send_slots.shape[-1]
    senders = send_slots.reshape(27, 1, each)
    down_turned = jnp.swapaxes(down_weight, 1, 2)

    smem = pl.BlockSpec(memory_space=pltpu.SMEM)
    vmem = pl.BlockSpec(memory_space=pltpu.VMEM)

    def params(mib):
        return pltpu.CompilerParams(vmem_limit_bytes=mib * MIB)

    outside = pl.BlockSpec(memory_space=pltpu.HBM)
    slab = slots // 3
    low, high, wide = pl.pallas_call(
        pack_kernel,
        out_shape=(
            jax.ShapeDtypeStruct((slab * 4, 128), BF16),
            jax.ShapeDtypeStruct((slab * 4, 128), BF16),
            jax.ShapeDtypeStruct(((count + 16) * 4, 128), F32),
        ),
        in_specs=[outside, outside],
        out_specs=(vmem,) * 3,
        scratch_shapes=[
            pltpu.SMEM(senders.shape, jnp.int32),
            pltpu.VMEM((count, width), BF16),
            pltpu.VMEM((slab * 4, 128), F32),
            pltpu.VMEM((slab * 4, 128), F32),
            pltpu.SemaphoreType.DMA((8,)),
            pltpu.SemaphoreType.DMA,
        ],
        compiler_params=params(14),
        name="pack",
    )(
        pltpu.with_memory_space_constraint(senders, pltpu.HBM),
        pltpu.with_memory_space_constraint(edge_state, pltpu.HBM),
    )
    middle = pl.pallas_call(
        pack_middle_kernel,
        out_shape=jax.ShapeDtypeStruct((slab * 4, 128), BF16),
        in_specs=[smem, vmem],
        out_specs=vmem,
        scratch_shapes=[pltpu.VMEM((slab * 4, 128), F32)],
        compiler_params=params(8),
        name="pack_middle",
    )(senders, wide)
    weights, bins, mixer, up_half, first_half, second_half, down_half, own_slots = pl.pallas_call(
        prepare_kernel,
        out_shape=(
            jax.ShapeDtypeStruct((quarter, 4 * neigh), BF16),
            jax.ShapeDtypeStruct((quarter, 4 * neigh), BF16),
            jax.ShapeDtypeStruct((2, angular * 4 * trip, 4 * trip), BF16),
            jax.ShapeDtypeStruct(up_weight.shape, BF16),
            jax.ShapeDtypeStruct(first_dense.shape, BF16),
            jax.ShapeDtypeStruct(second_dense.shape, BF16),
            jax.ShapeDtypeStruct(down_turned.shape, BF16),
            jax.ShapeDtypeStruct(senders.shape, jnp.int32),
        ),
        in_specs=[vmem] * 9,
        out_specs=(vmem,) * 8,
        compiler_params=params(16),
        name="prepare",
    )(
        angle_weight.T,
        angle_bins.T,
        live_lines,
        jnp.swapaxes(bilinear, 1, 2),
        up_weight,
        first_dense,
        second_dense,
        down_turned,
        senders,
    )
    hbm_slots = pltpu.with_memory_space_constraint(own_slots, pltpu.HBM)
    arrived = exchange((low, middle, high))

    reverse = pl.pallas_call(
        local_kernel,
        out_shape=jax.ShapeDtypeStruct((spare * 4, 128), F32),
        in_specs=[smem, smem, vmem, vmem],
        out_specs=vmem,
        scratch_shapes=[pltpu.VMEM((slots * 4, 128), F32)],
        compiler_params=params(16),
        name="reverse_local",
    )(fetch_index, own_slots, arrived[1], wide)

    triplet, *sending = pl.pallas_call(
        blocks_kernel,
        out_shape=(
            jax.ShapeDtypeStruct((spare, 2 * trip), F32),
        )
        + (jax.ShapeDtypeStruct((slab, 2 * trip), BF16),) * 3,
        in_specs=[outside] + [vmem] * 10,
        out_specs=(vmem,) * 4,
        scratch_shapes=[
            pltpu.VMEM((slots * 4, 128), F32),
            pltpu.VMEM((count, width), BF16),
            pltpu.VMEM((count, 4 * trip), BF16),
            pltpu.VMEM((quarter, angular * 4 * trip), BF16),
            pltpu.VMEM((slots, 2 * trip), F32),
            pltpu.VMEM((count, width), BF16),
            pltpu.VMEM((count, width), BF16),
            pltpu.SMEM(senders.shape, jnp.int32),
            pltpu.SemaphoreType.DMA,
        ],
        compiler_params=params(32),
        name="blocks",
    )(
        hbm_slots,
        arrived[0],
        arrived[2],
        reverse,
        weights,
        bins,
        down_half,
        mixer,
        up_half,
        first_half,
        second_half,
    )
    carried = exchange(sending)
    own_trip = pl.pallas_call(
        trip_kernel,
        out_shape=jax.ShapeDtypeStruct((count // 2, 2 * trip), F32),
        in_specs=[smem, vmem],
        out_specs=vmem,
        compiler_params=params(5),
        name="trip_local",
    )(fetch_index, triplet)
    own_trip = pl.pallas_call(
        trip_rest_kernel,
        out_shape=jax.ShapeDtypeStruct((spare, 2 * trip), F32),
        in_specs=[smem, vmem, vmem],
        out_specs=vmem,
        compiler_params=params(5),
        name="trip_rest",
    )(fetch_index, triplet, own_trip)
    own_trip = pl.pallas_call(
        trip_middle_kernel,
        out_shape=jax.ShapeDtypeStruct((spare, 2 * trip), F32),
        in_specs=[smem, vmem, vmem],
        out_specs=vmem,
        scratch_shapes=[pltpu.VMEM((slots, 2 * trip), F32)],
        compiler_params=params(5),
        name="trip_middle",
    )(own_slots, carried[1], own_trip)

    out = pl.pallas_call(
        final_kernel,
        out_shape=jax.ShapeDtypeStruct((count, width), BF16),
        in_specs=[outside] + [vmem] * 8,
        out_specs=outside,
        scratch_shapes=[pltpu.VMEM((slots, 2 * trip), F32)]
        + [pltpu.VMEM((count, width), BF16)] * 5
        + [pltpu.VMEM((count, 128), F32)]
        + [
            pltpu.SemaphoreType.DMA((8,)),
            pltpu.SMEM(senders.shape, jnp.int32),
            pltpu.SemaphoreType.DMA,
        ],
        compiler_params=params(24),
        name="final",
    )(
        hbm_slots,
        carried[0],
        carried[2],
        own_trip,
        edge_state,
        live_lines,
        up_half,
        first_half,
        second_half,
    )
    return out


def solution(mesh):
    spread = P(("gx", "gy", "gz"), None)
    in_specs = (
        spread,
        spread,
        spread,
        P("gx", "gy", "gz", None, None),
        P(("gx", "gy", "gz")),
        P(),
        P(),
        P(),
        P(),
        P(),
    )

    return jax.shard_map(local, mesh=mesh, in_specs=in_specs, out_specs=spread, check_vma=False)
```

```python
import jax
import jax.numpy as jnp
from jax import lax
from jax.experimental import pallas as pl
from jax.experimental.pallas import tpu as pltpu
from jax.sharding import PartitionSpec as P


HALF_ROOT = 0.7071067811865476
F32 = jnp.float32
BF16 = jnp.bfloat16
MIB = 1024 * 1024
BLOCK_TRIPS = 2
FINAL_TRIPS = 1


def silu_of_half(half):
    return half + half * jnp.tanh(half)


def dot(a, b):
    return jnp.dot(a, b, preferred_element_type=F32)


def dot_t(a, b):
    return lax.dot_general(a, b, (((1,), (1,)), ((), ())), preferred_element_type=F32)


def from_behind(array, axis, by):
    length = lax.axis_size(axis)
    return lax.ppermute(array, axis, [(i, (i + by) % length) for i in range(length)])


def second_kernel(low_ref, middle_ref, high_ref, *out_refs):
    third = low_ref.shape[0] // 3
    for a, slab_ref in enumerate((low_ref, middle_ref, high_ref)):
        for b, out_ref in enumerate(out_refs):
            out_ref[third * a : third * (a + 1), :] = slab_ref[third * b : third * (b + 1), :]


def third_kernel(low_ref, middle_ref, high_ref, *out_refs):
    rows = low_ref.shape[0] // 9
    for b, slab_ref in enumerate((low_ref, middle_ref, high_ref)):
        for a in range(3):
            for c, out_ref in enumerate(out_refs):
                source, target = rows * (3 * a + c), rows * (3 * b + a)
                out_ref[target : target + rows, :] = slab_ref[source : source + rows, :]


def exchange(slabs):
    vmem = pl.BlockSpec(memory_space=pltpu.VMEM)

    def regroup(kernel, pieces):
        return pl.pallas_call(
            kernel,
            out_shape=[jax.ShapeDtypeStruct(piece.shape, piece.dtype) for piece in pieces],
            in_specs=[vmem] * 3,
            out_specs=[vmem] * 3,
            compiler_params=pltpu.CompilerParams(vmem_limit_bytes=4 * MIB),
            name="regroup",
        )(*pieces)

    def hop(sent, axis):
        low, middle, high = sent
        return [from_behind(high, axis, 1), middle, from_behind(low, axis, -1)]

    slabs = hop(slabs, "gx")
    slabs = hop(regroup(second_kernel, slabs), "gy")
    return hop(regroup(third_kernel, slabs), "gz")


def pipelined(blocks, stages, trips):
    share = blocks // trips

    def trip(t, carry):
        for step in range(share + len(stages) - 1):
            for depth in reversed(range(len(stages))):
                if 0 <= step - depth < share:
                    stages[depth](t * share + step - depth)
        return carry

    if trips == 1:
        trip(0, 0)
    else:
        lax.fori_loop(0, trips, trip, 0)


def span(i, size):
    if isinstance(i, int):
        return slice(size * i, size * (i + 1))
    return pl.ds(pl.multiple_of(size * i, size), size)


def spread_rows(rows_ref, wide_ref, start, count, shift=0):
    for c in range(4):
        wide_ref[pl.ds(4 * (start + shift) + c, count, stride=4), :] = rows_ref[
            start : start + count, 128 * c : 128 * (c + 1)
        ].astype(F32)


def local_edge(fetch_ref, edge, spare):
    return jnp.minimum(fetch_ref[edge].astype(jnp.uint32), jnp.uint32(spare)).astype(jnp.int32)


def for_slots(send_ref, step, thirds=(0, 1, 2)):
    directions, _, each = send_ref.shape

    def body(i, carry):
        for c in thirds:
            t = 3 * i + c
            for r in range(each):
                step(t, r, t * each + r)
        return carry

    lax.fori_loop(0, directions // 3, body, 0)


def pack_slab(send_ref, wide_ref, packed_ref, out_ref, first):
    each = send_ref.shape[2]

    def body(i, carry):
        for r in range(each):
            source = pl.multiple_of(send_ref[first + i, 0, r] * 4 + 32, 4)
            target = pl.multiple_of((i * each + r) * 4, 4)
            packed_ref[pl.ds(target, 4), :] = wide_ref[pl.ds(source, 4), :]
        return carry

    lax.fori_loop(0, 9, body, 0)
    out_ref[...] = packed_ref[...].astype(BF16)


def pack_kernel(
    send_hbm_ref,
    rows_hbm_ref,
    low_ref,
    high_ref,
    wide_ref,
    send_ref,
    rows_ref,
    packed_low_ref,
    packed_high_ref,
    copied,
    listed,
):
    count = rows_ref.shape[0]
    chunk = count // 8
    copies = [
        pltpu.make_async_copy(
            rows_hbm_ref.at[pl.ds(chunk * i, chunk), :],
            rows_ref.at[pl.ds(chunk * i, chunk), :],
            copied.at[i],
        )
        for i in range(8)
    ]
    slots = pltpu.make_async_copy(send_hbm_ref, send_ref, listed)
    slots.start()
    wide_ref[0:32, :] = jnp.zeros((32, 128), F32)
    wide_ref[4 * count + 32 : 4 * count + 64, :] = jnp.zeros((32, 128), F32)
    for copy in copies:
        copy.start()
    for i, copy in enumerate(copies):
        copy.wait()
        spread_rows(rows_ref, wide_ref, chunk * i, chunk, 8)
    slots.wait()
    pack_slab(send_ref, wide_ref, packed_low_ref, low_ref, 0)
    pack_slab(send_ref, wide_ref, packed_high_ref, high_ref, 18)


def pack_middle_kernel(send_ref, wide_ref, out_ref, packed_ref):
    pack_slab(send_ref, wide_ref, packed_ref, out_ref, 9)


def place_wide(send_ref, arrived_ref, rows_ref, t, r, s):
    target = pl.multiple_of(send_ref[t, 0, r] * 4, 4)
    rows_ref[pl.ds(target, 4), :] = arrived_ref[pl.ds(pl.multiple_of(s * 4, 4), 4), :]


def local_kernel(fetch_ref, send_ref, middle_ref, wide_ref, out_ref, arrived32_ref):
    count = fetch_ref.shape[0]
    unroll = 32

    def body(i, carry):
        for k in range(unroll):
            edge = i * unroll + k
            source = pl.multiple_of(local_edge(fetch_ref, edge, count) * 4 + 32, 4)
            out_ref[pl.ds(pl.multiple_of(edge * 4, 4), 4), :] = wide_ref[pl.ds(source, 4), :]
        return carry

    lax.fori_loop(0, count // unroll, body, 0)
    widen_arrived(((1, middle_ref),), arrived32_ref)
    for_slots(send_ref, lambda t, r, s: place_wide(send_ref, arrived32_ref, out_ref, t, r, s), (1,))


def widen_arrived(pieces, wide_ref):
    for c, piece in pieces:
        rows = piece.shape[0] // 9
        for i in range(9):
            start = rows * (9 * (i % 3) + 3 * (i // 3) + c)
            wide_ref[start : start + rows, :] = piece[rows * i : rows * (i + 1), :].astype(F32)


def pick_slab(send_ref, trip_ref, packed_ref, out_ref, first):
    each = send_ref.shape[2]

    def body(i, carry):
        for r in range(each):
            source = send_ref[first + i, 0, r]
            packed_ref[pl.ds(i * each + r, 1), :] = trip_ref[pl.ds(source, 1), :]
        return carry

    lax.fori_loop(0, 9, body, 0)
    out_ref[...] = packed_ref[...].astype(BF16)


def blocks_kernel(
    send_hbm_ref,
    low_ref,
    high_ref,
    reverse_ref,
    weight_ref,
    bins_ref,
    down_ref,
    mixer_ref,
    up_ref,
    first_ref,
    second_ref,
    trip_ref,
    send_low_ref,
    send_high_ref,
    arrived32_ref,
    rows_ref,
    wide_ref,
    summed_ref,
    packed_low_ref,
    packed_high_ref,
    mixed_ref,
    inner_ref,
    send_ref,
    listed,
):
    count = rows_ref.shape[0]
    groups = summed_ref.shape[0] // 32
    trip = up_ref.shape[1]
    angular = summed_ref.shape[1] // 256
    listing = pltpu.make_async_copy(send_hbm_ref, send_ref, listed)
    listing.start()
    widen_arrived(((0, low_ref), (2, high_ref)), arrived32_ref)
    listing.wait()
    for_slots(
        send_ref,
        lambda t, r, s: place_wide(send_ref, arrived32_ref, reverse_ref, t, r, s),
        (0, 2),
    )
    for start in range(0, count, 256):
        for c in range(4):
            rows_ref[start : start + 256, 128 * c : 128 * (c + 1)] = reverse_ref[
                pl.ds(4 * start + c, 256, stride=4), :
            ].astype(BF16)
    trip_ref[count : count + 8, :] = jnp.zeros((8, 128), F32)
    step = 256
    shape = (step, 4 * trip)
    own_lanes = (
        lax.broadcasted_iota(jnp.int32, shape, 0) // 32 % 4
        == lax.broadcasted_iota(jnp.int32, shape, 1) // trip
    )
    downs = [jnp.concatenate([down_ref[block]] * 4, axis=0) for block in range(2)]

    def project(i, block):
        at = span(i, step)
        projected = silu_of_half(dot_t(rows_ref[at, :], downs[block]))
        wide_ref[at, :] = jnp.where(own_lanes, projected, 0.0).astype(BF16)

    def lift(i):
        at = span(i, step)
        lifted = silu_of_half(dot(trip_ref[at, :trip].astype(BF16), up_ref[0]))
        rows = rows_ref[at, :].astype(F32)
        mixed_ref[at, :] = ((rows + lifted) * HALF_ROOT).astype(BF16)

    def first(i):
        at = span(i, step)
        inner_ref[at, :] = silu_of_half(dot(mixed_ref[at, :], first_ref[0])).astype(BF16)

    def second(i):
        at = span(i, step)
        change = silu_of_half(dot(inner_ref[at, :], second_ref[0]))
        rows_ref[at, :] = ((mixed_ref[at, :].astype(F32) + change) * HALF_ROOT).astype(BF16)

    def group(g, carry):
        start = pl.multiple_of(g * 32, 32)
        weight = weight_ref[pl.ds(start, 32), :]
        bins = bins_ref[pl.ds(start, 32), :]
        zero = jnp.zeros_like(weight)
        chosen = [jnp.where(bins == b, weight, zero) for b in range(angular)]
        own = wide_ref[pl.ds(pl.multiple_of(g * 128, 128), 128), :]
        for q in range(0, angular, 8):
            sums = dot(jnp.concatenate(chosen[q : q + 8], axis=0), own).astype(BF16)
            for b in range(8):
                at = slice(256 * (q + b), 256 * (q + b + 1))
                summed_ref[pl.ds(start, 32), at] = sums[32 * b : 32 * (b + 1), :]
        return carry

    for i in range(count // step):
        project(i, 0)
    for block in range(2):
        lax.fori_loop(0, groups, group, 0, unroll=8)
        triplet = dot(summed_ref[...], mixer_ref[block]).astype(BF16).astype(F32)
        for g in range(groups):
            for a in range(4):
                start = 128 * g + 32 * a
                trip_ref[start : start + 32, trip * block : trip * (block + 1)] = triplet[
                    32 * g : 32 * (g + 1), trip * a : trip * (a + 1)
                ]
        if block == 0:
            pipelined(count // step, (lift, first, second, lambda i: project(i, 1)), BLOCK_TRIPS)

    pick_slab(send_ref, trip_ref, packed_low_ref, send_low_ref, 0)
    pick_slab(send_ref, trip_ref, packed_high_ref, send_high_ref, 18)


def gather_trips(fetch_ref, trip_ref, out_ref, start, count, spare):
    unroll = 32

    def body(i, carry):
        for k in range(unroll):
            edge = start + i * unroll + k
            out_ref[pl.ds(edge, 1), :] = trip_ref[pl.ds(local_edge(fetch_ref, edge, spare), 1), :]
        return carry

    lax.fori_loop(0, count // unroll, body, 0)


def trip_kernel(fetch_ref, send_ref, trip_ref, out_ref, middle_ref, packed_ref):
    pick_slab(send_ref, trip_ref, packed_ref, middle_ref, 9)
    gather_trips(fetch_ref, trip_ref, out_ref, 0, out_ref.shape[0], fetch_ref.shape[0])


def trip_rest_kernel(fetch_ref, trip_ref, begun_ref, out_ref):
    done, total = begun_ref.shape[0], out_ref.shape[0]
    out_ref[0:done, :] = begun_ref[...]
    gather_trips(fetch_ref, trip_ref, out_ref, done, total - done, fetch_ref.shape[0])


def trip_middle_kernel(
    fetch_ref, send_ref, middle_ref, trip_ref, begun_ref, out_ref, arrived32_ref
):
    count, done = fetch_ref.shape[0], begun_ref.shape[0]
    out_ref[0:done, :] = begun_ref[...]
    gather_trips(fetch_ref, trip_ref, out_ref, done, count - done, count)
    widen_arrived(((1, middle_ref),), arrived32_ref)

    def place(t, r, s):
        out_ref[pl.ds(send_ref[t, 0, r], 1), :] = arrived32_ref[pl.ds(s, 1), :]

    for_slots(send_ref, place, (1,))


def final_kernel(
    send_hbm_ref,
    low_ref,
    high_ref,
    trip_ref,
    rows_ref,
    live_ref,
    up_ref,
    first_ref,
    second_ref,
    out_ref,
    arrived32_ref,
    mixed_ref,
    inner_ref,
    mixed_next_ref,
    inner_next_ref,
    rows_out_ref,
    mask_ref,
    copied,
    send_ref,
    listed,
):
    count = rows_ref.shape[0]
    trip = up_ref.shape[1]
    listing = pltpu.make_async_copy(send_hbm_ref, send_ref, listed)
    listing.start()
    widen_arrived(((0, low_ref), (2, high_ref)), arrived32_ref)
    listing.wait()

    def place(t, r, s):
        trip_ref[pl.ds(send_ref[t, 0, r], 1), :] = arrived32_ref[pl.ds(s, 1), :]

    for_slots(send_ref, place, (0, 2))
    step = 512

    def lifted(at, block):
        both = trip_ref[at, :].astype(BF16)
        return silu_of_half(dot(both[:, trip * block : trip * (block + 1)], up_ref[block]))

    def lift(i):
        at = span(i, step)
        for g in range(i * (step // 128), (i + 1) * (step // 128)):
            line = live_ref[g : g + 1, :].astype(F32)
            mask_ref[span(g, 128), :] = jnp.broadcast_to(line, (128, 128)).T
        rows = rows_ref[at, :].astype(F32)
        mixed_ref[at, :] = ((rows + lifted(at, 0)) * HALF_ROOT).astype(BF16)

    def first(i):
        at = span(i, step)
        inner_ref[at, :] = silu_of_half(dot(mixed_ref[at, :], first_ref[0])).astype(BF16)

    def second(i):
        at = span(i, step)
        change = silu_of_half(dot(inner_ref[at, :], second_ref[0]))
        rows = (mixed_ref[at, :].astype(F32) + change) * HALF_ROOT
        mixed_next_ref[at, :] = ((rows + lifted(at, 1)) * HALF_ROOT).astype(BF16)

    def first_next(i):
        at = span(i, step)
        inner_next_ref[at, :] = silu_of_half(dot(mixed_next_ref[at, :], first_ref[1])).astype(BF16)

    def second_next(i):
        at = span(i, step)
        change = silu_of_half(dot(inner_next_ref[at, :], second_ref[1]))
        rows = (mixed_next_ref[at, :].astype(F32) + change) * HALF_ROOT
        for c in range(4):
            lanes = slice(128 * c, 128 * (c + 1))
            rows_out_ref[at, lanes] = jnp.where(mask_ref[at, :] >= 0.0, rows[:, lanes], 0.0).astype(
                BF16
            )
        copy_out(i).start()

    def copy_out(i):
        at = span(i, step)
        return pltpu.make_async_copy(rows_out_ref.at[at, :], out_ref.at[at, :], copied.at[i])

    pipelined(count // step, (lift, first, second, first_next, second_next), FINAL_TRIPS)
    for i in range(count // step):
        copy_out(i).wait()


def prepare_kernel(
    weight_ref,
    bins_ref,
    live_ref,
    bilinear_ref,
    up_ref,
    first_ref,
    second_ref,
    down_ref,
    senders_ref,
    weight_out_ref,
    bins_out_ref,
    mixer_ref,
    up_out_ref,
    first_out_ref,
    second_out_ref,
    down_out_ref,
    slots_ref,
):
    count = weight_ref.shape[1]
    slots_ref[...] = jnp.where(senders_ref[...] < 0, count, senders_ref[...])
    neigh = weight_ref.shape[0]
    side = 4 * neigh
    groups = weight_ref.shape[1] // side
    trip = bilinear_ref.shape[1]
    angular = bilinear_ref.shape[2] // trip
    row = lax.broadcasted_iota(jnp.int32, (side, side), 0)
    lane = lax.broadcasted_iota(jnp.int32, (side, side), 1)
    distinct = row % neigh != lane % neigh
    piece = lax.broadcasted_iota(jnp.int32, (neigh, side), 1) // neigh

    def turn(blocks):
        stacked = []
        for a in range(4):
            rows = jnp.zeros((neigh, side), F32)
            for h in range(4):
                shift = (h - a) * neigh % side
                moved = pltpu.roll(blocks[h], shift, 1) if shift else blocks[h]
                rows = jnp.where(piece == h, moved, rows)
            stacked.append(rows)
        return jnp.concatenate(stacked, axis=0).T

    for start in range(0, groups, 4):
        spans = [slice(side * (start + h), side * (start + h + 1)) for h in range(4)]
        rows = slice(neigh * start, neigh * start + side)
        weight_out_ref[rows, :] = turn([weight_ref[:, span] for span in spans]).astype(BF16)
        live = jnp.concatenate(
            [
                jnp.broadcast_to(live_ref[start + h : start + h + 1, :], (neigh, side))
                for h in range(4)
            ],
            axis=0,
        )
        bins = turn([bins_ref[:, span].astype(F32) for span in spans])
        bins_out_ref[rows, :] = jnp.where(distinct & (live >= 0), bins, -1.0).astype(BF16)
    lane_block = lax.broadcasted_iota(jnp.int32, (trip, 4 * trip), 1) // trip
    for block in range(2):
        turned = bilinear_ref[block].astype(F32).T
        wide = jnp.concatenate([turned] * 4, axis=1)
        for b in range(angular):
            part = wide[trip * b : trip * (b + 1), :]
            for a in range(4):
                start = 4 * trip * b + trip * a
                mixer_ref[block, start : start + trip, :] = jnp.where(
                    lane_block == a, part, 0.0
                ).astype(BF16)
    for source, target in (
        (up_ref, up_out_ref),
        (first_ref, first_out_ref),
        (second_ref, second_out_ref),
        (down_ref, down_out_ref),
    ):
        target[...] = (source[...].astype(F32) * 0.5).astype(BF16)


def local(
    edge_state,
    angle_weight,
    angle_bins,
    send_slots,
    fetch_index,
    down_weight,
    bilinear,
    up_weight,
    first_dense,
    second_dense,
):
    count, width = edge_state.shape
    neigh = angle_weight.shape[1]
    trip = down_weight.shape[2]
    angular = bilinear.shape[1] // trip
    slots = 27 * send_slots.shape[-1]
    quarter = count // 4
    groups = count // (4 * neigh)
    spare = count + 8
    live_lines = fetch_index.reshape(groups, 4 * neigh)
    each = send_slots.shape[-1]
    senders = send_slots.reshape(27, 1, each)
    down_turned = jnp.swapaxes(down_weight, 1, 2)

    smem = pl.BlockSpec(memory_space=pltpu.SMEM)
    vmem = pl.BlockSpec(memory_space=pltpu.VMEM)

    def params(mib):
        return pltpu.CompilerParams(vmem_limit_bytes=mib * MIB)

    outside = pl.BlockSpec(memory_space=pltpu.HBM)
    slab = slots // 3
    low, high, wide = pl.pallas_call(
        pack_kernel,
        out_shape=(
            jax.ShapeDtypeStruct((slab * 4, 128), BF16),
            jax.ShapeDtypeStruct((slab * 4, 128), BF16),
            jax.ShapeDtypeStruct(((count + 16) * 4, 128), F32),
        ),
        in_specs=[outside, outside],
        out_specs=(vmem,) * 3,
        scratch_shapes=[
            pltpu.SMEM(senders.shape, jnp.int32),
            pltpu.VMEM((count, width), BF16),
            pltpu.VMEM((slab * 4, 128), F32),
            pltpu.VMEM((slab * 4, 128), F32),
            pltpu.SemaphoreType.DMA((8,)),
            pltpu.SemaphoreType.DMA,
        ],
        compiler_params=params(14),
        name="pack",
    )(
        pltpu.with_memory_space_constraint(senders, pltpu.HBM),
        pltpu.with_memory_space_constraint(edge_state, pltpu.HBM),
    )
    middle = pl.pallas_call(
        pack_middle_kernel,
        out_shape=jax.ShapeDtypeStruct((slab * 4, 128), BF16),
        in_specs=[smem, vmem],
        out_specs=vmem,
        scratch_shapes=[pltpu.VMEM((slab * 4, 128), F32)],
        compiler_params=params(8),
        name="pack_middle",
    )(senders, wide)
    weights, bins, mixer, up_half, first_half, second_half, down_half, own_slots = pl.pallas_call(
        prepare_kernel,
        out_shape=(
            jax.ShapeDtypeStruct((quarter, 4 * neigh), BF16),
            jax.ShapeDtypeStruct((quarter, 4 * neigh), BF16),
            jax.ShapeDtypeStruct((2, angular * 4 * trip, 4 * trip), BF16),
            jax.ShapeDtypeStruct(up_weight.shape, BF16),
            jax.ShapeDtypeStruct(first_dense.shape, BF16),
            jax.ShapeDtypeStruct(second_dense.shape, BF16),
            jax.ShapeDtypeStruct(down_turned.shape, BF16),
            jax.ShapeDtypeStruct(senders.shape, jnp.int32),
        ),
        in_specs=[vmem] * 9,
        out_specs=(vmem,) * 8,
        compiler_params=params(16),
        name="prepare",
    )(
        angle_weight.T,
        angle_bins.T,
        live_lines,
        jnp.swapaxes(bilinear, 1, 2),
        up_weight,
        first_dense,
        second_dense,
        down_turned,
        senders,
    )
    hbm_slots = pltpu.with_memory_space_constraint(own_slots, pltpu.HBM)
    arrived = exchange((low, middle, high))

    reverse = pl.pallas_call(
        local_kernel,
        out_shape=jax.ShapeDtypeStruct((spare * 4, 128), F32),
        in_specs=[smem, smem, vmem, vmem],
        out_specs=vmem,
        scratch_shapes=[pltpu.VMEM((slots * 4, 128), F32)],
        compiler_params=params(16),
        name="reverse_local",
    )(fetch_index, own_slots, arrived[1], wide)

    triplet, send_low, send_high = pl.pallas_call(
        blocks_kernel,
        out_shape=(
            jax.ShapeDtypeStruct((spare, 2 * trip), F32),
        )
        + (jax.ShapeDtypeStruct((slab, 2 * trip), BF16),) * 2,
        in_specs=[outside] + [vmem] * 10,
        out_specs=(vmem,) * 3,
        scratch_shapes=[
            pltpu.VMEM((slots * 4, 128), F32),
            pltpu.VMEM((count, width), BF16),
            pltpu.VMEM((count, 4 * trip), BF16),
            pltpu.VMEM((quarter, angular * 4 * trip), BF16),
            pltpu.VMEM((slab, 2 * trip), F32),
            pltpu.VMEM((slab, 2 * trip), F32),
            pltpu.VMEM((count, width), BF16),
            pltpu.VMEM((count, width), BF16),
            pltpu.SMEM(senders.shape, jnp.int32),
            pltpu.SemaphoreType.DMA,
        ],
        compiler_params=params(32),
        name="blocks",
    )(
        hbm_slots,
        arrived[0],
        arrived[2],
        reverse,
        weights,
        bins,
        down_half,
        mixer,
        up_half,
        first_half,
        second_half,
    )
    own_trip, send_middle = pl.pallas_call(
        trip_kernel,
        out_shape=(
            jax.ShapeDtypeStruct((quarter, 2 * trip), F32),
            jax.ShapeDtypeStruct((slab, 2 * trip), BF16),
        ),
        in_specs=[smem, smem, vmem],
        out_specs=(vmem, vmem),
        scratch_shapes=[pltpu.VMEM((slab, 2 * trip), F32)],
        compiler_params=params(5),
        name="trip_local",
    )(fetch_index, own_slots, triplet)
    carried = exchange((send_low, send_middle, send_high))
    own_trip = pl.pallas_call(
        trip_rest_kernel,
        out_shape=jax.ShapeDtypeStruct((3 * quarter, 2 * trip), F32),
        in_specs=[smem, vmem, vmem],
        out_specs=vmem,
        compiler_params=params(5),
        name="trip_rest",
    )(fetch_index, triplet, own_trip)
    own_trip = pl.pallas_call(
        trip_middle_kernel,
        out_shape=jax.ShapeDtypeStruct((spare, 2 * trip), F32),
        in_specs=[smem, smem, vmem, vmem, vmem],
        out_specs=vmem,
        scratch_shapes=[pltpu.VMEM((slots, 2 * trip), F32)],
        compiler_params=params(6),
        name="trip_middle",
    )(fetch_index, own_slots, carried[1], triplet, own_trip)

    out = pl.pallas_call(
        final_kernel,
        out_shape=jax.ShapeDtypeStruct((count, width), BF16),
        in_specs=[outside] + [vmem] * 8,
        out_specs=outside,
        scratch_shapes=[pltpu.VMEM((slots, 2 * trip), F32)]
        + [pltpu.VMEM((count, width), BF16)] * 5
        + [pltpu.VMEM((count, 128), F32)]
        + [
            pltpu.SemaphoreType.DMA((8,)),
            pltpu.SMEM(senders.shape, jnp.int32),
            pltpu.SemaphoreType.DMA,
        ],
        compiler_params=params(24),
        name="final",
    )(
        hbm_slots,
        carried[0],
        carried[2],
        own_trip,
        edge_state,
        live_lines,
        up_half,
        first_half,
        second_half,
    )
    return out


def solution(mesh):
    spread = P(("gx", "gy", "gz"), None)
    in_specs = (
        spread,
        spread,
        spread,
        P("gx", "gy", "gz", None, None),
        P(("gx", "gy", "gz")),
        P(),
        P(),
        P(),
        P(),
        P(),
    )

    return jax.shard_map(local, mesh=mesh, in_specs=in_specs, out_specs=spread, check_vma=False)
```

```python
import jax
import jax.numpy as jnp
from jax import lax
from jax.experimental import pallas as pl
from jax.experimental.pallas import tpu as pltpu
from jax.sharding import PartitionSpec as P


HALF_ROOT = 0.7071067811865476
F32 = jnp.float32
BF16 = jnp.bfloat16
MIB = 1024 * 1024
BLOCK_TRIPS = 2
FINAL_TRIPS = 1


def silu_of_half(half):
    return half + half * jnp.tanh(half)


def dot(a, b):
    return jnp.dot(a, b, preferred_element_type=F32)


def dot_t(a, b):
    return lax.dot_general(a, b, (((1,), (1,)), ((), ())), preferred_element_type=F32)


def from_behind(array, axis, by):
    length = lax.axis_size(axis)
    return lax.ppermute(array, axis, [(i, (i + by) % length) for i in range(length)])


def second_kernel(low_ref, middle_ref, high_ref, *out_refs):
    third = low_ref.shape[0] // 3
    for a, slab_ref in enumerate((low_ref, middle_ref, high_ref)):
        for b, out_ref in enumerate(out_refs):
            out_ref[third * a : third * (a + 1), :] = slab_ref[third * b : third * (b + 1), :]


def third_kernel(low_ref, middle_ref, high_ref, *out_refs):
    rows = low_ref.shape[0] // 9
    for b, slab_ref in enumerate((low_ref, middle_ref, high_ref)):
        for a in range(3):
            for c, out_ref in enumerate(out_refs):
                source, target = rows * (3 * a + c), rows * (3 * b + a)
                out_ref[target : target + rows, :] = slab_ref[source : source + rows, :]


def second_split_kernel(low_ref, middle_ref, high_ref, *out_refs):
    outer_low_ref, outer_high_ref, own_ref, inner_low_ref, inner_high_ref = out_refs
    rows = low_ref.shape[0] // 9

    def copy(out_ref, i, slab_ref, j):
        out_ref[rows * i : rows * (i + 1), :] = slab_ref[rows * j : rows * (j + 1), :]

    for a, slab_ref in enumerate((low_ref, middle_ref, high_ref)):
        for c in range(3):
            copy(own_ref, 3 * a + c, slab_ref, 3 + c)
        for b, outer_ref, inner_ref in (
            (0, outer_low_ref, inner_low_ref),
            (2, outer_high_ref, inner_high_ref),
        ):
            copy(outer_ref, 2 * a, slab_ref, 3 * b)
            copy(outer_ref, 2 * a + 1, slab_ref, 3 * b + 2)
            copy(inner_ref, a, slab_ref, 3 * b + 1)


def third_split_kernel(low_ref, own_ref, high_ref, low_out_ref, high_out_ref):
    rows = own_ref.shape[0] // 9

    def copy(out_ref, i, slab_ref, j):
        out_ref[rows * i : rows * (i + 1), :] = slab_ref[rows * j : rows * (j + 1), :]

    for a in range(3):
        for c, out_ref in ((0, low_out_ref), (2, high_out_ref)):
            copy(out_ref, a, low_ref, 2 * a + c // 2)
            copy(out_ref, 3 + a, own_ref, 3 * a + c)
            copy(out_ref, 6 + a, high_ref, 2 * a + c // 2)


def middle_kernel(low_ref, own_ref, high_ref, out_ref):
    rows = own_ref.shape[0] // 9
    out_ref[0 : 3 * rows, :] = low_ref[...]
    out_ref[6 * rows : 9 * rows, :] = high_ref[...]
    for a in range(3):
        out_ref[rows * (3 + a) : rows * (4 + a), :] = own_ref[
            rows * (3 * a + 1) : rows * (3 * a + 2), :
        ]


def exchange(slabs, split=False):
    vmem = pl.BlockSpec(memory_space=pltpu.VMEM)
    rows, lanes = slabs[0].shape
    kind = slabs[0].dtype

    def regroup(kernel, pieces, counts):
        return pl.pallas_call(
            kernel,
            out_shape=[jax.ShapeDtypeStruct((rows * n // 9, lanes), kind) for n in counts],
            in_specs=[vmem] * 3,
            out_specs=[vmem] * len(counts),
            compiler_params=pltpu.CompilerParams(vmem_limit_bytes=4 * MIB),
            name="regroup",
        )(*pieces)

    def hop(low, high, axis):
        return from_behind(high, axis, 1), from_behind(low, axis, -1)

    from_low, from_high = hop(slabs[0], slabs[2], "gx")
    slabs = (from_low, slabs[1], from_high)
    if not split:
        low, own, high = regroup(second_kernel, slabs, (9, 9, 9))
        from_low, from_high = hop(low, high, "gy")
        low, middle, high = regroup(third_kernel, (from_low, own, from_high), (9, 9, 9))
        from_low, from_high = hop(low, high, "gz")
        return from_low, middle, from_high
    low, high, own, inner_low, inner_high = regroup(second_split_kernel, slabs, (6, 6, 9, 3, 3))
    from_low, from_high = hop(low, high, "gy")
    inner_low, inner_high = hop(inner_low, inner_high, "gy")
    low, high = regroup(third_split_kernel, (from_low, own, from_high), (9, 9))
    from_low, from_high = hop(low, high, "gz")
    middle = regroup(middle_kernel, (inner_low, own, inner_high), (9,))[0]
    return from_low, middle, from_high


def pipelined(blocks, stages, trips):
    share = blocks // trips

    def trip(t, carry):
        for step in range(share + len(stages) - 1):
            for depth in reversed(range(len(stages))):
                if 0 <= step - depth < share:
                    stages[depth](t * share + step - depth)
        return carry

    if trips == 1:
        trip(0, 0)
    else:
        lax.fori_loop(0, trips, trip, 0)


def span(i, size):
    if isinstance(i, int):
        return slice(size * i, size * (i + 1))
    return pl.ds(pl.multiple_of(size * i, size), size)


def spread_rows(rows_ref, wide_ref, start, count, shift=0):
    for c in range(4):
        wide_ref[pl.ds(4 * (start + shift) + c, count, stride=4), :] = rows_ref[
            start : start + count, 128 * c : 128 * (c + 1)
        ].astype(F32)


def local_edge(fetch_ref, edge, spare):
    return jnp.minimum(fetch_ref[edge].astype(jnp.uint32), jnp.uint32(spare)).astype(jnp.int32)


def for_slots(send_ref, step, thirds=(0, 1, 2)):
    directions, _, each = send_ref.shape

    def body(i, carry):
        for c in thirds:
            t = 3 * i + c
            for r in range(each):
                step(t, r, t * each + r)
        return carry

    lax.fori_loop(0, directions // 3, body, 0)


def pack_slab(send_ref, wide_ref, packed_ref, out_ref, first):
    each = send_ref.shape[2]

    def body(i, carry):
        for r in range(each):
            source = pl.multiple_of(send_ref[first + i, 0, r] * 4 + 32, 4)
            target = pl.multiple_of((i * each + r) * 4, 4)
            packed_ref[pl.ds(target, 4), :] = wide_ref[pl.ds(source, 4), :]
        return carry

    lax.fori_loop(0, 9, body, 0)
    out_ref[...] = packed_ref[...].astype(BF16)


def pack_kernel(
    send_hbm_ref,
    rows_hbm_ref,
    low_ref,
    high_ref,
    wide_ref,
    send_ref,
    rows_ref,
    packed_low_ref,
    packed_high_ref,
    copied,
    listed,
):
    count = rows_ref.shape[0]
    chunk = count // 8
    copies = [
        pltpu.make_async_copy(
            rows_hbm_ref.at[pl.ds(chunk * i, chunk), :],
            rows_ref.at[pl.ds(chunk * i, chunk), :],
            copied.at[i],
        )
        for i in range(8)
    ]
    slots = pltpu.make_async_copy(send_hbm_ref, send_ref, listed)
    slots.start()
    wide_ref[0:32, :] = jnp.zeros((32, 128), F32)
    wide_ref[4 * count + 32 : 4 * count + 64, :] = jnp.zeros((32, 128), F32)
    for copy in copies:
        copy.start()
    for i, copy in enumerate(copies):
        copy.wait()
        spread_rows(rows_ref, wide_ref, chunk * i, chunk, 8)
    slots.wait()
    pack_slab(send_ref, wide_ref, packed_low_ref, low_ref, 0)
    pack_slab(send_ref, wide_ref, packed_high_ref, high_ref, 18)


def pack_middle_kernel(send_ref, wide_ref, out_ref, packed_ref):
    pack_slab(send_ref, wide_ref, packed_ref, out_ref, 9)


def place_wide(send_ref, arrived_ref, rows_ref, t, r, s):
    target = pl.multiple_of(send_ref[t, 0, r] * 4, 4)
    rows_ref[pl.ds(target, 4), :] = arrived_ref[pl.ds(pl.multiple_of(s * 4, 4), 4), :]


def local_kernel(fetch_ref, send_ref, middle_ref, wide_ref, out_ref, arrived32_ref):
    count = fetch_ref.shape[0]
    unroll = 32

    def body(i, carry):
        for k in range(unroll):
            edge = i * unroll + k
            source = pl.multiple_of(local_edge(fetch_ref, edge, count) * 4 + 32, 4)
            out_ref[pl.ds(pl.multiple_of(edge * 4, 4), 4), :] = wide_ref[pl.ds(source, 4), :]
        return carry

    lax.fori_loop(0, count // unroll, body, 0)
    widen_arrived(((1, middle_ref),), arrived32_ref)
    for_slots(send_ref, lambda t, r, s: place_wide(send_ref, arrived32_ref, out_ref, t, r, s), (1,))


def widen_arrived(pieces, wide_ref):
    for c, piece in pieces:
        rows = piece.shape[0] // 9
        for i in range(9):
            start = rows * (9 * (i % 3) + 3 * (i // 3) + c)
            wide_ref[start : start + rows, :] = piece[rows * i : rows * (i + 1), :].astype(F32)


def pick_slab(send_ref, trip_ref, packed_ref, out_ref, first):
    each = send_ref.shape[2]

    def body(i, carry):
        for r in range(each):
            source = send_ref[first + i, 0, r]
            packed_ref[pl.ds(i * each + r, 1), :] = trip_ref[pl.ds(source, 1), :]
        return carry

    lax.fori_loop(0, 9, body, 0)
    out_ref[...] = packed_ref[...].astype(BF16)


def blocks_kernel(
    send_hbm_ref,
    low_ref,
    high_ref,
    reverse_ref,
    weight_ref,
    bins_ref,
    down_ref,
    mixer_ref,
    up_ref,
    first_ref,
    second_ref,
    trip_ref,
    send_low_ref,
    send_high_ref,
    arrived32_ref,
    rows_ref,
    wide_ref,
    summed_ref,
    packed_low_ref,
    packed_high_ref,
    mixed_ref,
    inner_ref,
    send_ref,
    listed,
):
    count = rows_ref.shape[0]
    groups = summed_ref.shape[0] // 32
    trip = up_ref.shape[1]
    angular = summed_ref.shape[1] // 256
    listing = pltpu.make_async_copy(send_hbm_ref, send_ref, listed)
    listing.start()
    widen_arrived(((0, low_ref), (2, high_ref)), arrived32_ref)
    listing.wait()
    for_slots(
        send_ref,
        lambda t, r, s: place_wide(send_ref, arrived32_ref, reverse_ref, t, r, s),
        (0, 2),
    )
    for start in range(0, count, 256):
        for c in range(4):
            rows_ref[start : start + 256, 128 * c : 128 * (c + 1)] = reverse_ref[
                pl.ds(4 * start + c, 256, stride=4), :
            ].astype(BF16)
    trip_ref[count : count + 8, :] = jnp.zeros((8, 128), F32)
    step = 256
    shape = (step, 4 * trip)
    own_lanes = (
        lax.broadcasted_iota(jnp.int32, shape, 0) // 32 % 4
        == lax.broadcasted_iota(jnp.int32, shape, 1) // trip
    )
    downs = [jnp.concatenate([down_ref[block]] * 4, axis=0) for block in range(2)]

    def project(i, block):
        at = span(i, step)
        projected = silu_of_half(dot_t(rows_ref[at, :], downs[block]))
        wide_ref[at, :] = jnp.where(own_lanes, projected, 0.0).astype(BF16)

    def lift(i):
        at = span(i, step)
        lifted = silu_of_half(dot(trip_ref[at, :trip].astype(BF16), up_ref[0]))
        rows = rows_ref[at, :].astype(F32)
        mixed_ref[at, :] = ((rows + lifted) * HALF_ROOT).astype(BF16)

    def first(i):
        at = span(i, step)
        inner_ref[at, :] = silu_of_half(dot(mixed_ref[at, :], first_ref[0])).astype(BF16)

    def second(i):
        at = span(i, step)
        change = silu_of_half(dot(inner_ref[at, :], second_ref[0]))
        rows_ref[at, :] = ((mixed_ref[at, :].astype(F32) + change) * HALF_ROOT).astype(BF16)

    def group(g, carry):
        start = pl.multiple_of(g * 32, 32)
        weight = weight_ref[pl.ds(start, 32), :]
        bins = bins_ref[pl.ds(start, 32), :]
        zero = jnp.zeros_like(weight)
        chosen = [jnp.where(bins == b, weight, zero) for b in range(angular)]
        own = wide_ref[pl.ds(pl.multiple_of(g * 128, 128), 128), :]
        for q in range(0, angular, 8):
            sums = dot(jnp.concatenate(chosen[q : q + 8], axis=0), own).astype(BF16)
            for b in range(8):
                at = slice(256 * (q + b), 256 * (q + b + 1))
                summed_ref[pl.ds(start, 32), at] = sums[32 * b : 32 * (b + 1), :]
        return carry

    for i in range(count // step):
        project(i, 0)
    for block in range(2):
        lax.fori_loop(0, groups, group, 0, unroll=8)
        triplet = dot(summed_ref[...], mixer_ref[block]).astype(BF16).astype(F32)
        for g in range(groups):
            for a in range(4):
                start = 128 * g + 32 * a
                trip_ref[start : start + 32, trip * block : trip * (block + 1)] = triplet[
                    32 * g : 32 * (g + 1), trip * a : trip * (a + 1)
                ]
        if block == 0:
            pipelined(count // step, (lift, first, second, lambda i: project(i, 1)), BLOCK_TRIPS)

    pick_slab(send_ref, trip_ref, packed_low_ref, send_low_ref, 0)
    pick_slab(send_ref, trip_ref, packed_high_ref, send_high_ref, 18)


def gather_trips(fetch_ref, trip_ref, out_ref, start, count, spare):
    unroll = 32

    def body(i, carry):
        for k in range(unroll):
            edge = start + i * unroll + k
            out_ref[pl.ds(edge, 1), :] = trip_ref[pl.ds(local_edge(fetch_ref, edge, spare), 1), :]
        return carry

    lax.fori_loop(0, count // unroll, body, 0)


def trip_kernel(fetch_ref, send_ref, trip_ref, out_ref, middle_ref, packed_ref):
    pick_slab(send_ref, trip_ref, packed_ref, middle_ref, 9)
    gather_trips(fetch_ref, trip_ref, out_ref, 0, out_ref.shape[0], fetch_ref.shape[0])


def trip_rest_kernel(fetch_ref, trip_ref, begun_ref, out_ref):
    done, total = begun_ref.shape[0], out_ref.shape[0]
    out_ref[0:done, :] = begun_ref[...]
    gather_trips(fetch_ref, trip_ref, out_ref, done, total - done, fetch_ref.shape[0])


def trip_middle_kernel(
    fetch_ref, send_ref, middle_ref, trip_ref, begun_ref, out_ref, arrived32_ref
):
    count, done = fetch_ref.shape[0], begun_ref.shape[0]
    out_ref[0:done, :] = begun_ref[...]
    gather_trips(fetch_ref, trip_ref, out_ref, done, count - done, count)
    widen_arrived(((1, middle_ref),), arrived32_ref)

    def place(t, r, s):
        out_ref[pl.ds(send_ref[t, 0, r], 1), :] = arrived32_ref[pl.ds(s, 1), :]

    for_slots(send_ref, place, (1,))


def final_kernel(
    send_hbm_ref,
    low_ref,
    high_ref,
    trip_ref,
    rows_ref,
    live_ref,
    up_ref,
    first_ref,
    second_ref,
    out_ref,
    arrived32_ref,
    mixed_ref,
    inner_ref,
    mixed_next_ref,
    inner_next_ref,
    rows_out_ref,
    mask_ref,
    copied,
    send_ref,
    listed,
):
    count = rows_ref.shape[0]
    trip = up_ref.shape[1]
    listing = pltpu.make_async_copy(send_hbm_ref, send_ref, listed)
    listing.start()
    widen_arrived(((0, low_ref), (2, high_ref)), arrived32_ref)
    listing.wait()

    def place(t, r, s):
        trip_ref[pl.ds(send_ref[t, 0, r], 1), :] = arrived32_ref[pl.ds(s, 1), :]

    for_slots(send_ref, place, (0, 2))
    step = 512

    def lifted(at, block):
        both = trip_ref[at, :].astype(BF16)
        return silu_of_half(dot(both[:, trip * block : trip * (block + 1)], up_ref[block]))

    def lift(i):
        at = span(i, step)
        for g in range(i * (step // 128), (i + 1) * (step // 128)):
            line = live_ref[g : g + 1, :].astype(F32)
            mask_ref[span(g, 128), :] = jnp.broadcast_to(line, (128, 128)).T
        rows = rows_ref[at, :].astype(F32)
        mixed_ref[at, :] = ((rows + lifted(at, 0)) * HALF_ROOT).astype(BF16)

    def first(i):
        at = span(i, step)
        inner_ref[at, :] = silu_of_half(dot(mixed_ref[at, :], first_ref[0])).astype(BF16)

    def second(i):
        at = span(i, step)
        change = silu_of_half(dot(inner_ref[at, :], second_ref[0]))
        rows = (mixed_ref[at, :].astype(F32) + change) * HALF_ROOT
        mixed_next_ref[at, :] = ((rows + lifted(at, 1)) * HALF_ROOT).astype(BF16)

    def first_next(i):
        at = span(i, step)
        inner_next_ref[at, :] = silu_of_half(dot(mixed_next_ref[at, :], first_ref[1])).astype(BF16)

    def second_next(i):
        at = span(i, step)
        change = silu_of_half(dot(inner_next_ref[at, :], second_ref[1]))
        rows = (mixed_next_ref[at, :].astype(F32) + change) * HALF_ROOT
        for c in range(4):
            lanes = slice(128 * c, 128 * (c + 1))
            rows_out_ref[at, lanes] = jnp.where(mask_ref[at, :] >= 0.0, rows[:, lanes], 0.0).astype(
                BF16
            )
        copy_out(i).start()

    def copy_out(i):
        at = span(i, step)
        return pltpu.make_async_copy(rows_out_ref.at[at, :], out_ref.at[at, :], copied.at[i])

    pipelined(count // step, (lift, first, second, first_next, second_next), FINAL_TRIPS)
    for i in range(count // step):
        copy_out(i).wait()


def prepare_kernel(
    weight_ref,
    bins_ref,
    live_ref,
    bilinear_ref,
    up_ref,
    first_ref,
    second_ref,
    down_ref,
    senders_ref,
    weight_out_ref,
    bins_out_ref,
    mixer_ref,
    up_out_ref,
    first_out_ref,
    second_out_ref,
    down_out_ref,
    slots_ref,
):
    count = weight_ref.shape[1]
    slots_ref[...] = jnp.where(senders_ref[...] < 0, count, senders_ref[...])
    neigh = weight_ref.shape[0]
    side = 4 * neigh
    groups = weight_ref.shape[1] // side
    trip = bilinear_ref.shape[1]
    angular = bilinear_ref.shape[2] // trip
    row = lax.broadcasted_iota(jnp.int32, (side, side), 0)
    lane = lax.broadcasted_iota(jnp.int32, (side, side), 1)
    distinct = row % neigh != lane % neigh
    piece = lax.broadcasted_iota(jnp.int32, (neigh, side), 1) // neigh

    def turn(blocks):
        stacked = []
        for a in range(4):
            rows = jnp.zeros((neigh, side), F32)
            for h in range(4):
                shift = (h - a) * neigh % side
                moved = pltpu.roll(blocks[h], shift, 1) if shift else blocks[h]
                rows = jnp.where(piece == h, moved, rows)
            stacked.append(rows)
        return jnp.concatenate(stacked, axis=0).T

    for start in range(0, groups, 4):
        spans = [slice(side * (start + h), side * (start + h + 1)) for h in range(4)]
        rows = slice(neigh * start, neigh * start + side)
        weight_out_ref[rows, :] = turn([weight_ref[:, span] for span in spans]).astype(BF16)
        live = jnp.concatenate(
            [
                jnp.broadcast_to(live_ref[start + h : start + h + 1, :], (neigh, side))
                for h in range(4)
            ],
            axis=0,
        )
        bins = turn([bins_ref[:, span].astype(F32) for span in spans])
        bins_out_ref[rows, :] = jnp.where(distinct & (live >= 0), bins, -1.0).astype(BF16)
    lane_block = lax.broadcasted_iota(jnp.int32, (trip, 4 * trip), 1) // trip
    for block in range(2):
        turned = bilinear_ref[block].astype(F32).T
        wide = jnp.concatenate([turned] * 4, axis=1)
        for b in range(angular):
            part = wide[trip * b : trip * (b + 1), :]
            for a in range(4):
                start = 4 * trip * b + trip * a
                mixer_ref[block, start : start + trip, :] = jnp.where(
                    lane_block == a, part, 0.0
                ).astype(BF16)
    for source, target in (
        (up_ref, up_out_ref),
        (first_ref, first_out_ref),
        (second_ref, second_out_ref),
        (down_ref, down_out_ref),
    ):
        target[...] = (source[...].astype(F32) * 0.5).astype(BF16)


def local(
    edge_state,
    angle_weight,
    angle_bins,
    send_slots,
    fetch_index,
    down_weight,
    bilinear,
    up_weight,
    first_dense,
    second_dense,
):
    count, width = edge_state.shape
    neigh = angle_weight.shape[1]
    trip = down_weight.shape[2]
    angular = bilinear.shape[1] // trip
    slots = 27 * send_slots.shape[-1]
    quarter = count // 4
    groups = count // (4 * neigh)
    spare = count + 8
    live_lines = fetch_index.reshape(groups, 4 * neigh)
    each = send_slots.shape[-1]
    senders = send_slots.reshape(27, 1, each)
    down_turned = jnp.swapaxes(down_weight, 1, 2)

    smem = pl.BlockSpec(memory_space=pltpu.SMEM)
    vmem = pl.BlockSpec(memory_space=pltpu.VMEM)

    def params(mib):
        return pltpu.CompilerParams(vmem_limit_bytes=mib * MIB)

    outside = pl.BlockSpec(memory_space=pltpu.HBM)
    slab = slots // 3
    low, high, wide = pl.pallas_call(
        pack_kernel,
        out_shape=(
            jax.ShapeDtypeStruct((slab * 4, 128), BF16),
            jax.ShapeDtypeStruct((slab * 4, 128), BF16),
            jax.ShapeDtypeStruct(((count + 16) * 4, 128), F32),
        ),
        in_specs=[outside, outside],
        out_specs=(vmem,) * 3,
        scratch_shapes=[
            pltpu.SMEM(senders.shape, jnp.int32),
            pltpu.VMEM((count, width), BF16),
            pltpu.VMEM((slab * 4, 128), F32),
            pltpu.VMEM((slab * 4, 128), F32),
            pltpu.SemaphoreType.DMA((8,)),
            pltpu.SemaphoreType.DMA,
        ],
        compiler_params=params(14),
        name="pack",
    )(
        pltpu.with_memory_space_constraint(senders, pltpu.HBM),
        pltpu.with_memory_space_constraint(edge_state, pltpu.HBM),
    )
    middle = pl.pallas_call(
        pack_middle_kernel,
        out_shape=jax.ShapeDtypeStruct((slab * 4, 128), BF16),
        in_specs=[smem, vmem],
        out_specs=vmem,
        scratch_shapes=[pltpu.VMEM((slab * 4, 128), F32)],
        compiler_params=params(8),
        name="pack_middle",
    )(senders, wide)
    weights, bins, mixer, up_half, first_half, second_half, down_half, own_slots = pl.pallas_call(
        prepare_kernel,
        out_shape=(
            jax.ShapeDtypeStruct((quarter, 4 * neigh), BF16),
            jax.ShapeDtypeStruct((quarter, 4 * neigh), BF16),
            jax.ShapeDtypeStruct((2, angular * 4 * trip, 4 * trip), BF16),
            jax.ShapeDtypeStruct(up_weight.shape, BF16),
            jax.ShapeDtypeStruct(first_dense.shape, BF16),
            jax.ShapeDtypeStruct(second_dense.shape, BF16),
            jax.ShapeDtypeStruct(down_turned.shape, BF16),
            jax.ShapeDtypeStruct(senders.shape, jnp.int32),
        ),
        in_specs=[vmem] * 9,
        out_specs=(vmem,) * 8,
        compiler_params=params(16),
        name="prepare",
    )(
        angle_weight.T,
        angle_bins.T,
        live_lines,
        jnp.swapaxes(bilinear, 1, 2),
        up_weight,
        first_dense,
        second_dense,
        down_turned,
        senders,
    )
    hbm_slots = pltpu.with_memory_space_constraint(own_slots, pltpu.HBM)
    arrived = exchange((low, middle, high), True)

    reverse = pl.pallas_call(
        local_kernel,
        out_shape=jax.ShapeDtypeStruct((spare * 4, 128), F32),
        in_specs=[smem, smem, vmem, vmem],
        out_specs=vmem,
        scratch_shapes=[pltpu.VMEM((slots * 4, 128), F32)],
        compiler_params=params(16),
        name="reverse_local",
    )(fetch_index, own_slots, arrived[1], wide)

    triplet, send_low, send_high = pl.pallas_call(
        blocks_kernel,
        out_shape=(
            jax.ShapeDtypeStruct((spare, 2 * trip), F32),
        )
        + (jax.ShapeDtypeStruct((slab, 2 * trip), BF16),) * 2,
        in_specs=[outside] + [vmem] * 10,
        out_specs=(vmem,) * 3,
        scratch_shapes=[
            pltpu.VMEM((slots * 4, 128), F32),
            pltpu.VMEM((count, width), BF16),
            pltpu.VMEM((count, 4 * trip), BF16),
            pltpu.VMEM((quarter, angular * 4 * trip), BF16),
            pltpu.VMEM((slab, 2 * trip), F32),
            pltpu.VMEM((slab, 2 * trip), F32),
            pltpu.VMEM((count, width), BF16),
            pltpu.VMEM((count, width), BF16),
            pltpu.SMEM(senders.shape, jnp.int32),
            pltpu.SemaphoreType.DMA,
        ],
        compiler_params=params(32),
        name="blocks",
    )(
        hbm_slots,
        arrived[0],
        arrived[2],
        reverse,
        weights,
        bins,
        down_half,
        mixer,
        up_half,
        first_half,
        second_half,
    )
    own_trip, send_middle = pl.pallas_call(
        trip_kernel,
        out_shape=(
            jax.ShapeDtypeStruct((quarter, 2 * trip), F32),
            jax.ShapeDtypeStruct((slab, 2 * trip), BF16),
        ),
        in_specs=[smem, smem, vmem],
        out_specs=(vmem, vmem),
        scratch_shapes=[pltpu.VMEM((slab, 2 * trip), F32)],
        compiler_params=params(5),
        name="trip_local",
    )(fetch_index, own_slots, triplet)
    carried = exchange((send_low, send_middle, send_high))
    own_trip = pl.pallas_call(
        trip_rest_kernel,
        out_shape=jax.ShapeDtypeStruct((3 * quarter, 2 * trip), F32),
        in_specs=[smem, vmem, vmem],
        out_specs=vmem,
        compiler_params=params(5),
        name="trip_rest",
    )(fetch_index, triplet, own_trip)
    own_trip = pl.pallas_call(
        trip_middle_kernel,
        out_shape=jax.ShapeDtypeStruct((spare, 2 * trip), F32),
        in_specs=[smem, smem, vmem, vmem, vmem],
        out_specs=vmem,
        scratch_shapes=[pltpu.VMEM((slots, 2 * trip), F32)],
        compiler_params=params(6),
        name="trip_middle",
    )(fetch_index, own_slots, carried[1], triplet, own_trip)

    out = pl.pallas_call(
        final_kernel,
        out_shape=jax.ShapeDtypeStruct((count, width), BF16),
        in_specs=[outside] + [vmem] * 8,
        out_specs=outside,
        scratch_shapes=[pltpu.VMEM((slots, 2 * trip), F32)]
        + [pltpu.VMEM((count, width), BF16)] * 5
        + [pltpu.VMEM((count, 128), F32)]
        + [
            pltpu.SemaphoreType.DMA((8,)),
            pltpu.SMEM(senders.shape, jnp.int32),
            pltpu.SemaphoreType.DMA,
        ],
        compiler_params=params(24),
        name="final",
    )(
        hbm_slots,
        carried[0],
        carried[2],
        own_trip,
        edge_state,
        live_lines,
        up_half,
        first_half,
        second_half,
    )
    return out


def solution(mesh):
    spread = P(("gx", "gy", "gz"), None)
    in_specs = (
        spread,
        spread,
        spread,
        P("gx", "gy", "gz", None, None),
        P(("gx", "gy", "gz")),
        P(),
        P(),
        P(),
        P(),
        P(),
    )

    return jax.shard_map(local, mesh=mesh, in_specs=in_specs, out_specs=spread, check_vma=False)
```
